256 devices in a mesh: row: 16 (over z, core), col: 16 (over x, y).
Axes of the slice: x: 4, y: 4, z: 8, core: 2. Of those that a mesh axis runs over, the one named last changes fastest.
Arguments:
- attn_out: bfloat16 [6, 4096, 2048], P(None, 'col', 'row'), may hold values from -0.25 to 0.25
- out_cotangent: bfloat16 [6, 4096, 2048], P(None, 'row', 'col'), may hold values from -6 to 6
- frozen: bfloat16 [6, 2048, 2048], P(None, 'row', 'col'), may hold values from -0.5 to 0.5
- adapt_in: bfloat16 [6, 32, 2048], P(None, None, 'row'), may hold values from -0.125 to 0.125
- adapt_out: bfloat16 [6, 32, 2048], P(None, None, 'col'), may hold values from -1 to 1
- magnitude: float32 [6, 2048], P(None, 'col'), may hold values from 0.1 to 1.9
Outputs:
- input_grad: bfloat16 [6, 4096, 2048], P(None, 'col', 'row')
- adapt_in_grad: float32 [6, 32, 2048], P(None, None, 'row')
- adapt_out_grad: float32 [6, 32, 2048], P(None, None, 'col')
- magnitude_grad: float32 [6, 2048], P(None, 'col')
The draws below stay inside these ranges and needn't reach their ends.
All inputs are finite; a program needn't handle non-finite values.
Results may differ from the reference program's by a relative error of at most 0.0065.
Values may be sent and summed in bfloat16 or wider, within the bound.
A program may use at most 64 MiB of HBM per device.

```python
import jax
import jax.numpy as jnp
from jax import lax

WIDTH = 2048
IN_WIDTH = 2048
RANK = 32
LAYERS = 6
TOKENS = 4096


def steps_of(key, extent, shards, smallest, top_value):
    def one(dim, shards_of):
        steps = jax.random.uniform(jax.random.fold_in(jax.random.fold_in(key, 6), dim), (shards_of,), jnp.float32, smallest / len(shards), top_value / len(shards))
        return jnp.repeat(jnp.exp(steps), extent[dim] // shards_of).reshape((-1,) + (1,) * (len(extent) - dim - 1))

    level = one(*shards[0])
    for cut in shards[1:]:
        level = level * one(*cut)
    return level


def gaussian(rng, extent, spread, reach, split=(), kind=jnp.bfloat16):
    level = steps_of(rng, extent, split, -0.22, 0.18) if split else 1.0
    entries = jax.random.normal(rng, extent, jnp.float32) * spread * level
    return jnp.minimum(jnp.maximum(entries, -reach), reach).astype(kind)


def setup_inputs(seed: int = 0) -> dict:
    key_list = jax.random.split(jax.random.key(seed), 7)
    attn_out = gaussian(key_list[0], (LAYERS, TOKENS, IN_WIDTH), (TOKENS ** -0.5), 0.25, ((1, 16), (2, 16)))
    out_cotangent = gaussian(key_list[1], (LAYERS, TOKENS, WIDTH), 1.0, 6.0, ((1, 16), (2, 16)))
    frozen = gaussian(key_list[2], (LAYERS, IN_WIDTH, WIDTH), (IN_WIDTH // 16) ** -0.5, 0.5, ((1, 16), (2, 16)))
    adapt_in = gaussian(key_list[3], (LAYERS, RANK, IN_WIDTH), IN_WIDTH ** -0.5, 0.125, ((2, 16),))
    adapt_out = gaussian(key_list[4], (LAYERS, RANK, WIDTH), RANK ** -0.5, 1.0, ((2, 16),))
    magnitude = jnp.clip(1.0 + 0.18 * jax.random.normal(key_list[5], (LAYERS, WIDTH), jnp.float32), 0.1, 1.9)
    return {"attn_out": attn_out, "out_cotangent": out_cotangent, "frozen": frozen, "adapt_in": adapt_in, "adapt_out": adapt_out, "magnitude": magnitude}


precise = lax.Precision.HIGHEST

def one_layer(acts, grads, frozen, adapt_in, adapt_out, magnitude):
    merged = frozen.astype(jnp.float32) + lax.dot_general(adapt_in, adapt_out, (((0,), (0,)), ((), ())), preferred_element_type=jnp.float32)
    squares = lax.optimization_barrier(jnp.sum(merged * merged, axis=0))
    norms = jnp.sqrt(squares + 0.25)
    outer = lax.dot_general(acts, grads, (((0,), (0,)), ((), ())), preferred_element_type=jnp.float32)
    dots = lax.optimization_barrier(jnp.sum(merged * outer, axis=0))
    scales = magnitude / norms
    correct = -magnitude * dots / (norms * norms * norms)
    magnitude_grad = dots / norms
    delta = outer * scales + merged * correct
    in_grad = lax.dot_general(adapt_out.astype(jnp.float32), delta, (((1,), (1,)), ((), ())), precision=precise)
    out_grad = jnp.dot(adapt_in.astype(jnp.float32), delta, precision=precise)
    scaled = (grads * scales).astype(jnp.bfloat16)
    weight_low = merged.astype(jnp.bfloat16)
    input_grad = lax.dot_general(scaled, weight_low, (((1,), (1,)), ((), ())), preferred_element_type=jnp.float32).astype(jnp.bfloat16)
    return (input_grad, in_grad, out_grad, magnitude_grad)

def reference(attn_out, out_cotangent, frozen, adapt_in, adapt_out, magnitude):
    results = [one_layer(attn_out[layer_at], out_cotangent[layer_at], frozen[layer_at], adapt_in[layer_at], adapt_out[layer_at], magnitude[layer_at]) for layer_at in range(LAYERS)]
    return (jnp.stack([item[0] for item in results]), jnp.stack([item[1] for item in results]), jnp.stack([item[2] for item in results]), jnp.stack([item[3] for item in results]))
```

```python
import functools

import jax
import jax.numpy as jnp
from jax import lax
from jax.experimental import pallas as pl
from jax.experimental.pallas import tpu as pltpu
from jax.sharding import PartitionSpec as P

F32 = jnp.float32
BF16 = jnp.bfloat16
HIGH = lax.Precision.HIGHEST
N = 16
ZS = 8
L = 6
NG = 3
GL = L // NG
CH = 512
NCH = 2048 // CH


def nn(a, b):
    return lax.dot_general(a, b, (((1,), (0,)), ((), ())), preferred_element_type=F32)


def nt(a, b):
    return lax.dot_general(a, b, (((1,), (1,)), ((), ())), preferred_element_type=F32)


def tn(a, b):
    return lax.dot_general(a, b, (((0,), (0,)), ((), ())), preferred_element_type=F32)


def exact(a, b):
    return lax.dot_general(a, b, (((1,), (0,)), ((), ())), precision=HIGH, preferred_element_type=F32)


def aligned(i, n):
    return pl.multiple_of(i * n, n)


def kernel(
    acts, grads, ain, mag, frozen, aout,
    o_in, o_ain, o_aout, o_mag,
    H, G, WA, MF, WM, SQ, SC, CR, PPb, PPr, PSb, PD, USb, USr, DL, D1r, D2r, OGr, IPf, IRr, IAr,
    in_s, t1s, t1r, t2s, t2r, rs, rr, ls, lr, ds, dr, ws, wr,
    sqs, sqr, scs, scr, p1s, p1r, p2s, p2r, pbs, pbr, uss, usr,
    d1s, d1r, d2s, d2r, d3s, d3r, ogs, ogr, irs, irr, ias, iar,
):
    r = lax.axis_index("row")
    c = lax.axis_index("col")
    z, k = r // 2, r % 2
    x, y = c // 4, c % 4

    def rcopy(src, dst, ss, rsem, **ids):
        return pltpu.make_async_remote_copy(
            src_ref=src, dst_ref=dst, send_sem=ss, recv_sem=rsem,
            device_id=ids, device_id_type=pl.DeviceIdType.MESH,
        )

    def landed(ref, sem):
        pltpu.make_async_copy(ref, ref, sem).wait()

    def to_row(make):
        def step(i, _):
            make(lax.rem(r + i, N)).start()
            return 0
        lax.fori_loop(1, N, step, 0)

    def to_col(make):
        def step(i, _):
            make(lax.rem(c + i, N)).start()
            return 0
        lax.fori_loop(1, N, step, 0)

    own = pl.ds(aligned(c, 128), 128)
    cf = pltpu.make_async_copy(frozen, WA.at[:, 0:128, own], in_s.at[0])
    ca = pltpu.make_async_copy(aout, WA.at[:, 128:160, own], in_s.at[1])
    cf.start()
    ca.start()

    barrier = pltpu.get_barrier_semaphore()

    def greet(i, _):
        pl.semaphore_signal(barrier, inc=1, device_id={"row": lax.rem(r + i, N)}, device_id_type=pl.DeviceIdType.MESH)
        pl.semaphore_signal(barrier, inc=1, device_id={"col": lax.rem(c + i, N)}, device_id_type=pl.DeviceIdType.MESH)
        return 0

    lax.fori_loop(1, N, greet, 0)
    pl.semaphore_wait(barrier, 2 * (N - 1))

    def layers(g):
        return pl.ds(GL * g, GL)

    for g in range(NG):
        to_row(lambda p, g=g: rcopy(
            grads.at[layers(g), pl.ds(aligned(p, 16), 16), :], H.at[r, layers(g)],
            t1s.at[g], t1r.at[g], row=p))
    H[r] = grads[:, pl.ds(aligned(r, 16), 16), :]

    cf.wait()
    ca.wait()

    def place_of(h, a, b):
        return 4 * b + a if h == 0 else 4 * a + b

    pos = ((y, x), (x, y))

    def wblock(h, a, b, lo=0, hi=160):
        return WA.at[pl.ds(3 * h, 3), lo:hi, pl.ds(aligned(place_of(h, a, b), 128), 128)]

    def mod4(i):
        return lax.rem(i + 4, 4)

    def w_copy(h, kind, slot, a, b, target):
        lo, hi = ((0, 160), (0, 160), (0, 80), (80, 160))[kind]
        ref = wblock(h, a, b, lo, hi)
        return rcopy(ref, ref, ws.at[h, slot, kind], wr.at[h, slot, kind], col=target)

    def first(h, kind, j):
        a, b = pos[h]
        step = 1 if kind in (0, 2) else -1
        return w_copy(h, kind, 0, mod4(a + j), b, place_of(h, mod4(a + step), b))

    def second(h, kind, slot, j, jb):
        a, b = pos[h]
        step = 1 if kind in (0, 2) else -1
        return w_copy(h, kind, slot, mod4(a + j), mod4(b + jb), place_of(h, a, mod4(b + step)))

    def first_landed(h, kind):
        a, b = pos[h]
        j = (-1, 1, 2, 2)[kind]
        lo, hi = ((0, 160), (0, 160), (0, 80), (80, 160))[kind]
        landed(wblock(h, mod4(a + j), b, lo, hi), wr.at[h, 0, kind])

    def second_landed(h, kind, slot, j):
        a, b = pos[h]
        jb = (-1, 1, 2, 2)[kind]
        lo, hi = ((0, 160), (0, 160), (0, 80), (80, 160))[kind]
        landed(wblock(h, mod4(a + j), mod4(b + jb), lo, hi), wr.at[h, slot, kind])

    offsets = ((1, 0), (2, -1), (3, 1), (4, 2))

    def second_out(h, slot, j):
        second(h, 0, slot, j, 0).start()
        second(h, 1, slot, j, 0).start()

    def second_on(h, slot, j):
        second_landed(h, 0, slot, j)
        second(h, 2, slot, j, -1).start()
        second_landed(h, 1, slot, j)
        second(h, 3, slot, j, 1).start()

    for h in range(2):
        first(h, 0, 0).start()
        first(h, 1, 0).start()
    for h in range(2):
        second_out(h, 1, 0)

    rows = lax.broadcasted_iota(jnp.int32, (256, 32), 0)
    ranks = lax.broadcasted_iota(jnp.int32, (256, 32), 1)

    def spread(i):
        off = rows % 16 - 2 * i
        return jnp.where((off >= 0) & (off < 2) & (ranks == rows // 16 * 2 + off), 1.0, 0.0).astype(F32)

    back_rows = lax.broadcasted_iota(jnp.int32, (32, 256), 1)
    back_ranks = lax.broadcasted_iota(jnp.int32, (32, 256), 0)

    def collect(i):
        off = back_rows % 16 - 2 * i
        return jnp.where((off >= 0) & (off < 2) & (back_ranks == back_rows // 16 * 2 + off), 1.0, 0.0).astype(F32)

    SQ[...] = jnp.zeros((8, 128), F32)
    part = jnp.zeros((256, 256), F32)
    inner = jnp.zeros((256, 128), F32)
    for i in range(L):
        block = WA[i, 0:128, own].astype(F32) + tn(ain[i], WA[i, 128:160, own])
        SQ[i : i + 1] = jnp.sum(block * block, axis=0, keepdims=True)
        wide = nn(spread(i).astype(BF16), ain[i]).astype(BF16)
        part += nt(wide, acts[i])
        high = block.astype(BF16)
        inner += nn(wide, high) + nn(wide, (block - high.astype(F32)).astype(BF16))
    PPb[...] = part.astype(BF16).reshape(N, 16, 256)
    USb[:, 16:32, :] = inner.astype(BF16).reshape(N, 16, 128)
    SQr = SQ_all = D2r.at[1]
    SQr[r] = SQ[...]
    to_row(lambda p: rcopy(SQ, SQ_all.at[r], sqs, sqr, row=p))
    PPr[r] = PPb[r]
    to_row(lambda p: rcopy(PPb.at[p], PPr.at[r], p1s, p1r, row=p))

    for g in range(NG):
        landed(H.at[0 : N - 1, layers(g)], t1r.at[g])
        mine = pl.ds(aligned(r, 16), 16)
        to_col(lambda q, g=g: rcopy(
            H.at[q, layers(g)], G.at[layers(g), pl.ds(aligned(r, 16), 16), pl.ds(aligned(c, 128), 128)],
            t2s.at[g], t2r.at[g], col=q))
        G[GL * g : GL * g + GL, mine, own] = H[c, GL * g : GL * g + GL]

    for h in range(2):
        first_landed(h, 0)
        first(h, 2, -1).start()
        second_out(h, 2, -1)
        first_landed(h, 1)
        first(h, 3, 1).start()
        second_out(h, 3, 1)

    landed(SQ_all.at[0 : N - 1], sqr)
    squares = SQr[0]
    for p in range(1, N):
        squares = squares + SQr[p]
    norms = jnp.sqrt(squares[0:L] + 0.25)
    scales = mag[...] / norms

    landed(PPr.at[0 : N - 1], p1r)
    total = PPr[0].astype(F32)
    for p in range(1, N):
        total = total + PPr[p].astype(F32)
    PSb[...] = total.astype(BF16)

    def chunk(g, q, count=GL, at=0):
        return G.at[pl.ds(GL * g + at, count), pl.ds(aligned(q, 16), 16), :]

    def across(i):
        return lax.rem(z + i + ZS, ZS) * 2 + k

    def right(g, s):
        ref = chunk(g, across(-s)) if s < 3 else chunk(g, across(-s), 1, 0)
        return rcopy(ref, ref, rs.at[g, s], rr.at[g, s], row=across(1))

    def left(g, s):
        ref = chunk(g, across(s)) if s < 3 else chunk(g, across(s), 1, 1)
        return rcopy(ref, ref, ls.at[g, s], lr.at[g, s], row=across(-1))

    partner = z * 2 + 1 - k

    def over(g, n, i):
        ref = chunk(g, across(i))
        return rcopy(ref, ref, ds.at[g, n], dr.at[g, n], row=partner)

    hops = (0, -1, -2, -3, 1, 2, 3, 4)

    def ring(g, s):
        if s == 0:
            landed(G.at[layers(g), pl.ds(aligned(r, 16), 16), 0 : 128 * (N - 1)], t2r.at[g])
            right(g, 0).start()
            left(g, 0).start()
            over(g, 0, 0).start()
        elif s < 4:
            landed(chunk(g, across(-s)), rr.at[g, s - 1])
            right(g, s).start()
            landed(chunk(g, across(s)), lr.at[g, s - 1])
            left(g, s).start()
            over(g, s, -s).start()
            over(g, 3 + s, s).start()
        else:
            landed(chunk(g, across(4), 1, 0), rr.at[g, 3])
            landed(chunk(g, across(4), 1, 1), lr.at[g, 3])
            over(g, 7, 4).start()

    def ring_landed(g):
        for n, i in enumerate(hops):
            landed(chunk(g, lax.rem(z + i + ZS, ZS) * 2 + 1 - k), dr.at[g, n])

    ring(0, 0)

    for i in range(L):
        SC[i : i + 1, own] = scales[i : i + 1]
    SCs = SQ
    landed(SQr.at[0 : N - 1], sqs)
    SCs[0:L] = scales
    to_col(lambda q: rcopy(SCs, SC.at[:, own], scs, scr, col=q))

    @pl.when(c != r)
    def _():
        rcopy(PSb, PD.at[r], p2s, p2r, row=c).start()

    @pl.when(c == r)
    def _():
        PD[r] = PSb[...]

    ring(1, 0)
    ring(0, 1)
    ring(2, 0)

    for h in range(2):
        second_on(h, 1, 0)
    for h in range(2):
        first_landed(h, 2)
        first_landed(h, 3)
        second_out(h, 4, 2)

    ring(1, 1)
    ring(0, 2)

    @pl.when(c == r)
    def _():
        landed(PD.at[0 : N - 1], p2r)
        to_col(lambda q: rcopy(PD, PD, pbs.at[lax.rem(q - c + N, N)], pbr, col=q))

    for h in range(2):
        second_on(h, 2, -1)
        second_on(h, 3, 1)

    ring(2, 1)
    ring(1, 2)
    ring(0, 3)

    @pl.when(c != r)
    def _():
        landed(PD, pbr)

    kind = lax.broadcasted_iota(jnp.int32, (256, 128), 0) % 16 // 2
    low = PD[...].reshape(N * 16, 256)
    inner_outer = jnp.zeros((256, 128), F32)
    for i in range(L):
        inner_outer = jnp.where(kind == i, nn(low, grads[i]), inner_outer)
    USb[:, 0:16, :] = inner_outer.astype(BF16).reshape(N, 16, 128)
    USr[r] = USb[r]
    to_row(lambda p: rcopy(USb.at[p], USr.at[r], uss, usr, row=p))

    for h in range(2):
        second_on(h, 4, 2)

    ring(2, 2)
    ring(1, 3)
    ring(0, 4)

    for h in range(2):
        for slot, j in offsets:
            second_landed(h, 2, slot, j)
            second_landed(h, 3, slot, j)

    landed(D1r.at[0 : N - 1], scr)

    def prepare(i):
        for n in range(NCH):
            cols = pl.ds(n * CH, CH)
            merged = WA[i, 0:128, cols].astype(F32) + tn(ain[i], WA[i, 128:160, cols])
            MF[i, :, cols] = merged
            WM[i, :, cols] = merged.astype(BF16)

    DL[...] = jnp.zeros((8, 2048), F32)

    def dots_of(i):
        for n in range(NCH):
            cols = pl.ds(n * CH, CH)
            outer = tn(acts[i], G[i, :, cols])
            DL[i : i + 1, cols] = jnp.sum(MF[i, :, cols] * outer, axis=0, keepdims=True)

    def grads_of(i):
        got = jnp.zeros((256, 128), F32)
        low_t = jnp.zeros((32, 256), F32)
        for n in range(NCH):
            cols = pl.ds(n * CH, CH)
            scaled = (G[i, :, cols].astype(F32) * SC[i : i + 1, cols]).astype(BF16)
            got += nt(scaled, WM[i, :, cols])
            low_t += nt(WA[i, 128:160, cols], scaled)
        o_in[i] = got.astype(BF16)
        high = low_t.astype(BF16)
        rest = (low_t - high.astype(F32)).astype(BF16)
        return nn(high, acts[i]) + nn(rest, acts[i])

    for i in range(L):
        prepare(i)
    ring(2, 3)
    ring(1, 4)

    in_part = jnp.zeros((256, 128), F32)

    def placed(i, x):
        return exact(spread(i), x)

    for i in range(0, GL):
        if i == 0:
            ring_landed(0)
        dots_of(i)
        in_part += placed(i, grads_of(i))
    ring(2, 4)
    ring_landed(1)
    for i in range(GL, 2 * GL):
        dots_of(i)
        in_part += placed(i, grads_of(i))
    ring_landed(2)
    for i in range(2 * GL, L):
        dots_of(i)

    D1r[c] = DL[:, own]
    to_col(lambda q: rcopy(DL.at[:, pl.ds(aligned(q, 128), 128)], D1r.at[c], d1s, d1r, col=q))
    for i in range(2 * GL, L):
        in_part += placed(i, grads_of(i))
    IPf[...] = in_part.reshape(N, 16, 128)
    IRr[c] = IPf[c]
    to_col(lambda q: rcopy(IPf.at[q], IRr.at[c], irs, irr, col=q))

    landed(D1r.at[0 : N - 1], d1r)
    sub = D1r[0]
    for p in range(1, N):
        sub = sub + D1r[p]
    landed(SQr.at[0 : N - 1], scs)
    SQ[...] = sub
    D2 = D2r.at[0]
    D2[r] = sub
    to_row(lambda p: rcopy(SQ, D2.at[r], d2s, d2r, row=p))

    landed(USr.at[0 : N - 1], usr)
    both = USr[0].astype(F32)
    for p in range(1, N):
        both = both + USr[p].astype(F32)

    landed(IRr.at[0 : N - 1], irr)
    in_sum = IRr[0]
    for p in range(1, N):
        in_sum = in_sum + IRr[p]
    IAr[c] = in_sum
    to_col(lambda q: rcopy(IAr.at[c], IAr.at[c], ias, iar, col=q))

    landed(D2.at[0 : N - 1], d2r)
    dots8 = D2[0]
    for p in range(1, N):
        dots8 = dots8 + D2[p]
    dots = dots8[0:L]
    o_mag[...] = dots / norms
    correct = -mag[...] * dots / (norms * norms * norms)
    for i in range(L):
        CR[i : i + 1, own] = correct[i : i + 1]
    landed(D1r.at[0 : N - 1], d1s)
    landed(D2.at[0 : N - 1], d2s)
    SQ[0:L] = correct
    to_col(lambda q: rcopy(SQ, CR.at[:, own], d3s, d3r, col=q))
    out = jnp.zeros((16, 128), F32)
    kind16 = lax.broadcasted_iota(jnp.int32, (16, 128), 0) // 2
    for i in range(L):
        out = jnp.where(kind16 == i, both[0:16] * scales[i : i + 1] + both[16:32] * correct[i : i + 1], out)
    OGr[r] = out
    to_row(lambda p: rcopy(OGr.at[r], OGr.at[r], ogs, ogr, row=p))

    landed(D1r.at[0 : N - 1], d3r)
    landed(IAr.at[0 : N - 1], iar)
    in_all = IAr[...].reshape(N * 16, 128)
    for i in range(L):
        second_term = jnp.zeros((32, 128), F32)
        for n in range(NCH):
            cols = pl.ds(n * CH, CH)
            scaled_out = WA[i, 128:160, cols].astype(F32) * CR[i : i + 1, cols]
            high = scaled_out.astype(BF16)
            rest = (scaled_out - high.astype(F32)).astype(BF16)
            second_term += nt(high, WM[i, :, cols]) + nt(rest, WM[i, :, cols])
        o_ain[i] = exact(collect(i), in_all) + second_term

    landed(OGr.at[0 : N - 1], ogr)
    out_all = OGr[...].reshape(N * 16, 128)
    for i in range(L):
        o_aout[i] = exact(collect(i), out_all)

    for g in range(NG):
        landed(H.at[0 : N - 1, layers(g)], t1s.at[g])
        landed(H.at[0 : N - 1, layers(g)], t2s.at[g])
        for s in range(4):
            right(g, s).wait_send()
            left(g, s).wait_send()
        for n, i in enumerate(hops):
            over(g, n, i).wait_send()
    for h in range(2):
        for n, j in enumerate((0, 0, -1, 1)):
            first(h, n, j).wait_send()
        for slot, j in offsets:
            for n, jb in enumerate((0, 0, -1, 1)):
                second(h, n, slot, j, jb).wait_send()
    landed(PPr.at[0 : N - 1], p1s)
    landed(USr.at[0 : N - 1], uss)
    landed(D1r.at[0 : N - 1], d3s)
    landed(OGr.at[0 : N - 1], ogs)
    landed(IRr.at[0 : N - 1], irs)
    landed(IAr.at[0 : N - 1], ias)

    @pl.when(c != r)
    def _():
        landed(PSb, p2s)

    @pl.when(c == r)
    def _():
        def drain(i, _):
            landed(PD, pbs.at[i])
            return 0
        lax.fori_loop(1, N, drain, 0)


def body(attn_out, out_cotangent, frozen, adapt_in, adapt_out, magnitude):
    dma = pltpu.SemaphoreType.DMA
    vmem = pl.BlockSpec(memory_space=pltpu.VMEM)
    anywhere = pl.BlockSpec(memory_space=pl.ANY)
    V = pltpu.VMEM
    scratch = [
        V((N, L, 16, 128), BF16),
        V((L, 256, 2048), BF16),
        V((L, 160, 2048), BF16),
        V((L, 128, 2048), F32),
        V((L, 128, 2048), BF16),
        V((8, 128), F32),
        V((8, 2048), F32),
        V((8, 2048), F32),
        V((N, 16, 256), BF16),
        V((N, 16, 256), BF16),
        V((16, 256), BF16),
        V((N, 16, 256), BF16),
        V((N, 32, 128), BF16),
        V((N, 32, 128), BF16),
        V((8, 2048), F32),
        V((N, 8, 128), F32),
        V((2, N, 8, 128), F32),
        V((N, 16, 128), F32),
        V((N, 16, 128), F32),
        V((N, 16, 128), F32),
        V((N, 16, 128), F32),
        dma((2,)),
        dma((NG,)), dma((NG,)), dma((NG,)), dma((NG,)),
        dma((NG, 4)), dma((NG, 4)), dma((NG, 4)), dma((NG, 4)),
        dma((NG, 8)), dma((NG, 8)),
        dma((2, 5, 4)), dma((2, 5, 4)),
        dma, dma, dma, dma, dma, dma, dma, dma,
        dma((N,)), dma, dma, dma,
        dma, dma, dma, dma, dma, dma, dma, dma, dma, dma, dma, dma,
    ]
    return pl.pallas_call(
        kernel,
        out_shape=(
            jax.ShapeDtypeStruct((L, 256, 128), BF16),
            jax.ShapeDtypeStruct((L, 32, 128), F32),
            jax.ShapeDtypeStruct((L, 32, 128), F32),
            jax.ShapeDtypeStruct((L, 128), F32),
        ),
        in_specs=[vmem, vmem, vmem, vmem, anywhere, anywhere],
        out_specs=(vmem, vmem, vmem, vmem),
        scratch_shapes=scratch,
        compiler_params=pltpu.CompilerParams(
            collective_id=0, has_side_effects=True, vmem_limit_bytes=48 * 1024 * 1024
        ),
        name="dora",
    )(attn_out, out_cotangent, adapt_in, magnitude, frozen, adapt_out)


def solution(mesh):
    return jax.shard_map(
        body,
        mesh=mesh,
        in_specs=(
            P(None, "col", "row"),
            P(None, "row", "col"),
            P(None, "row", "col"),
            P(None, None, "row"),
            P(None, None, "col"),
            P(None, "col"),
        ),
        out_specs=(
            P(None, "col", "row"),
            P(None, None, "row"),
            P(None, None, "col"),
            P(None, "col"),
        ),
        check_vma=False,
    )
```

```python
import functools

import jax
import jax.numpy as jnp
from jax import lax
from jax.experimental import pallas as pl
from jax.experimental.pallas import tpu as pltpu
from jax.sharding import PartitionSpec as P

F32 = jnp.float32
BF16 = jnp.bfloat16
HIGH = lax.Precision.HIGHEST
N = 16
ZS = 8
L = 6
NG = 3
GL = L // NG
CH = 512
NCH = 2048 // CH


def nn(a, b):
    return lax.dot_general(a, b, (((1,), (0,)), ((), ())), preferred_element_type=F32)


def nt(a, b):
    return lax.dot_general(a, b, (((1,), (1,)), ((), ())), preferred_element_type=F32)


def tn(a, b):
    return lax.dot_general(a, b, (((0,), (0,)), ((), ())), preferred_element_type=F32)


def exact(a, b):
    return lax.dot_general(a, b, (((1,), (0,)), ((), ())), precision=HIGH, preferred_element_type=F32)


def aligned(i, n):
    return pl.multiple_of(i * n, n)


def kernel(
    h_acts, h_grads, h_ain, h_mag, h_frozen, h_aout,
    h_in, h_ain_grad, h_aout_grad, h_mag_grad,
    acts, grads, ain, mag, o_in, o_ain, o_aout, o_mag,
    H, G, WA, MF, WM, SQ, SQr, SC, CR, PPb, PPr, PSb, PD, PE, USb, USr, DL, D1r, D2r, OGr, IPf, IRr, IAr,
    in_s, out_s, t1s, t1r, t2s, t2r, rs, rr, ls, lr, ds, dr, ws, wr,
    sqs, sqr, scs, scr, p1s, p1r, p2s, p2r, pbs, pbr, uss, usr,
    d1s, d1r, d2s, d2r, d3s, d3r, ogs, ogr, irs, irr, ias, iar,
):
    r = lax.axis_index("row")
    c = lax.axis_index("col")
    z, k = r // 2, r % 2
    x, y = c // 4, c % 4
    scope = jax.named_scope

    def rcopy(src, dst, ss, rsem, **ids):
        return pltpu.make_async_remote_copy(
            src_ref=src, dst_ref=dst, send_sem=ss, recv_sem=rsem,
            device_id=ids, device_id_type=pl.DeviceIdType.MESH,
        )

    def landed(ref, sem):
        pltpu.make_async_copy(ref, ref, sem).wait()

    def to_row(make):
        def step(i, _):
            make(lax.rem(r + i, N)).start()
            return 0
        lax.fori_loop(1, N, step, 0)

    def to_col(make):
        def step(i, _):
            make(lax.rem(c + i, N)).start()
            return 0
        lax.fori_loop(1, N, step, 0)

    own = pl.ds(aligned(c, 128), 128)
    mine = pl.ds(aligned(r, 16), 16)

    def layers(g):
        return pl.ds(GL * g, GL)

    loads = [
        pltpu.make_async_copy(h_grads, grads, in_s.at[0]),
        pltpu.make_async_copy(h_frozen, WA.at[:, 0:128, own], in_s.at[1]),
        pltpu.make_async_copy(h_aout, WA.at[:, 128:160, own], in_s.at[2]),
        pltpu.make_async_copy(h_ain, ain, in_s.at[3]),
        pltpu.make_async_copy(h_acts, acts, in_s.at[4]),
        pltpu.make_async_copy(h_mag, mag, in_s.at[5]),
    ]
    with scope("s00_barrier"):
        barrier = pltpu.get_barrier_semaphore()

        def greet(i, _):
            pl.semaphore_signal(barrier, inc=1, device_id={"row": lax.rem(r + i, N)}, device_id_type=pl.DeviceIdType.MESH)
            pl.semaphore_signal(barrier, inc=1, device_id={"col": lax.rem(c + i, N)}, device_id_type=pl.DeviceIdType.MESH)
            return 0

        lax.fori_loop(1, N, greet, 0)
        for load in loads:
            load.start()
        for load in loads:
            load.wait()
        H[r] = grads[:, mine, :]
        pl.semaphore_wait(barrier, 2 * (N - 1))

    with scope("s01_t1send"):
        for g in range(NG):
            to_row(lambda p, g=g: rcopy(
                grads.at[layers(g), pl.ds(aligned(p, 16), 16), :], H.at[r, layers(g)],
                t1s.at[g], t1r.at[g], row=p))

    def place_of(h, a, b):
        return 4 * b + a if h == 0 else 4 * a + b

    pos = ((y, x), (x, y))
    cuts = ((0, 160), (0, 160), (0, 80), (80, 160))

    def wblock(h, a, b, lo=0, hi=160):
        return WA.at[pl.ds(3 * h, 3), lo:hi, pl.ds(aligned(place_of(h, a, b), 128), 128)]

    def mod4(i):
        return lax.rem(i + 4, 4)

    def w_copy(h, kind, slot, a, b, target):
        ref = wblock(h, a, b, *cuts[kind])
        return rcopy(ref, ref, ws.at[h, slot, kind], wr.at[h, slot, kind], col=target)

    def first(h, kind, j):
        a, b = pos[h]
        step = 1 if kind in (0, 2) else -1
        return w_copy(h, kind, 0, mod4(a + j), b, place_of(h, mod4(a + step), b))

    def second(h, kind, slot, j, jb):
        a, b = pos[h]
        step = 1 if kind in (0, 2) else -1
        return w_copy(h, kind, slot, mod4(a + j), mod4(b + jb), place_of(h, a, mod4(b + step)))

    def first_landed(h, kind):
        a, b = pos[h]
        landed(wblock(h, mod4(a + (-1, 1, 2, 2)[kind]), b, *cuts[kind]), wr.at[h, 0, kind])

    def second_landed(h, kind, slot, j):
        a, b = pos[h]
        landed(wblock(h, mod4(a + j), mod4(b + (-1, 1, 2, 2)[kind]), *cuts[kind]), wr.at[h, slot, kind])

    offsets = ((1, 0), (2, -1), (3, 1), (4, 2))

    def second_out(h, slot, j):
        second(h, 0, slot, j, 0).start()
        second(h, 1, slot, j, 0).start()

    def second_on(slot):
        with scope(f"w_on{slot}"):
            j = dict(offsets)[slot]
            for h in range(2):
                second_landed(h, 0, slot, j)
                second(h, 2, slot, j, -1).start()
                second_landed(h, 1, slot, j)
                second(h, 3, slot, j, 1).start()

    for h in range(2):
        first(h, 0, 0).start()
        first(h, 1, 0).start()
    for h in range(2):
        second_out(h, 1, 0)

    rows = lax.broadcasted_iota(jnp.int32, (256, 32), 0)
    ranks = lax.broadcasted_iota(jnp.int32, (256, 32), 1)

    def spread(i):
        off = rows % 16 - 2 * i
        return jnp.where((off >= 0) & (off < 2) & (ranks == rows // 16 * 2 + off), 1.0, 0.0).astype(F32)

    back_rows = lax.broadcasted_iota(jnp.int32, (32, 256), 1)
    back_ranks = lax.broadcasted_iota(jnp.int32, (32, 256), 0)

    def collect(i):
        off = back_rows % 16 - 2 * i
        return jnp.where((off >= 0) & (off < 2) & (back_ranks == back_rows // 16 * 2 + off), 1.0, 0.0).astype(F32)

    with scope("s02_local"):
        SQ[...] = jnp.zeros((8, 128), F32)
        part = jnp.zeros((256, 256), F32)
        inner = jnp.zeros((256, 128), F32)
        for i in range(L):
            block = WA[i, 0:128, own].astype(F32) + tn(ain[i], WA[i, 128:160, own])
            SQ[i : i + 1] = jnp.sum(block * block, axis=0, keepdims=True)
            wide = nn(spread(i).astype(BF16), ain[i]).astype(BF16)
            part += nt(wide, acts[i])
            high = block.astype(BF16)
            inner += nn(wide, high) + nn(wide, (block - high.astype(F32)).astype(BF16))
        PPb[...] = part.astype(BF16).reshape(N, 16, 256)
        USb[:, 16:32, :] = inner.astype(BF16).reshape(N, 16, 128)
        SQr[r] = SQ[...]
        to_row(lambda p: rcopy(SQ, SQr.at[r], sqs, sqr, row=p))
        PPr[r] = PPb[r]
        to_row(lambda p: rcopy(PPb.at[p], PPr.at[r], p1s, p1r, row=p))

    def exchange(g):
        with scope(f"t2_{g}"):
            landed(H.at[0 : N - 1, layers(g)], t1r.at[g])
            to_col(lambda q: rcopy(
                H.at[q, layers(g)], G.at[layers(g), mine, own], t2s.at[g], t2r.at[g], col=q))
            G[GL * g : GL * g + GL, mine, own] = H[c, GL * g : GL * g + GL]

    def chunk(g, q, count=GL, at=0):
        return G.at[pl.ds(GL * g + at, count), pl.ds(aligned(q, 16), 16), :]

    def across(i):
        return lax.rem(z + i + ZS, ZS) * 2 + k

    def right(g, s):
        ref = chunk(g, across(-s)) if s < 3 else chunk(g, across(-s), 1, 0)
        return rcopy(ref, ref, rs.at[g, s], rr.at[g, s], row=across(1))

    def left(g, s):
        ref = chunk(g, across(s)) if s < 3 else chunk(g, across(s), 1, 1)
        return rcopy(ref, ref, ls.at[g, s], lr.at[g, s], row=across(-1))

    partner = z * 2 + 1 - k

    def over(g, n, i):
        ref = chunk(g, across(i))
        return rcopy(ref, ref, ds.at[g, n], dr.at[g, n], row=partner)

    hops = (0, -1, -2, -3, 1, 2, 3, 4)

    def ring(g, s):
        with scope(f"r{g}{s}"):
            if s == 0:
                landed(G.at[layers(g), mine, 0 : 128 * (N - 1)], t2r.at[g])
                right(g, 0).start()
                left(g, 0).start()
                over(g, 0, 0).start()
            elif s < 4:
                landed(chunk(g, across(-s)), rr.at[g, s - 1])
                right(g, s).start()
                landed(chunk(g, across(s)), lr.at[g, s - 1])
                left(g, s).start()
                over(g, s, -s).start()
                over(g, 3 + s, s).start()
            else:
                landed(chunk(g, across(4), 1, 0), rr.at[g, 3])
                landed(chunk(g, across(4), 1, 1), lr.at[g, 3])
                over(g, 7, 4).start()

    def ring_landed(g):
        with scope(f"r{g}_landed"):
            for n, i in enumerate(hops):
                landed(chunk(g, lax.rem(z + i + ZS, ZS) * 2 + 1 - k), dr.at[g, n])

    def prepare(i):
        with scope(f"prep{i}"):
            for n in range(NCH):
                cols = pl.ds(n * CH, CH)
                merged = WA[i, 0:128, cols].astype(F32) + tn(ain[i], WA[i, 128:160, cols])
                MF[i, :, cols] = merged
                WM[i, :, cols] = merged.astype(BF16)

    def dots_of(i):
        with scope(f"dots{i}"):
            for n in range(NCH):
                cols = pl.ds(n * CH, CH)
                outer = tn(acts[i], G[i, :, cols])
                DL[i : i + 1, cols] = jnp.sum(MF[i, :, cols] * outer, axis=0, keepdims=True)

    def grads_of(i):
        with scope(f"grads{i}"):
            got = jnp.zeros((256, 128), F32)
            low_t = jnp.zeros((32, 256), F32)
            for n in range(NCH):
                cols = pl.ds(n * CH, CH)
                scaled = (G[i, :, cols].astype(F32) * SC[i : i + 1, cols]).astype(BF16)
                got += nt(scaled, WM[i, :, cols])
                low_t += nt(WA[i, 128:160, cols], scaled)
            o_in[i] = got.astype(BF16)
            high = low_t.astype(BF16)
            rest = (low_t - high.astype(F32)).astype(BF16)
            new = exact(spread(i), nn(high, acts[i]) + nn(rest, acts[i])).reshape(N, 16, 128)
            IPf[...] = new if i == 0 else IPf[...] + new

    DL[...] = jnp.zeros((8, 2048), F32)

    exchange(0)
    exchange(1)
    ring(0, 0)
    exchange(2)

    with scope("w_first"):
        for h in range(2):
            first_landed(h, 0)
            first(h, 2, -1).start()
            second_out(h, 2, -1)
            first_landed(h, 1)
            first(h, 3, 1).start()
            second_out(h, 3, 1)

    ring(1, 0)

    with scope("norms"):
        landed(SQr.at[0 : N - 1], sqr)
        squares = SQr[0]
        for p in range(1, N):
            squares = squares + SQr[p]
        norms = jnp.sqrt(squares[0:L] + 0.25)
        scales = mag[...] / norms
        for i in range(L):
            SC[i : i + 1, own] = scales[i : i + 1]
        landed(SQr.at[0 : N - 1], sqs)
        SQ[0:L] = scales
        to_col(lambda q: rcopy(SQ, SC.at[:, own], scs, scr, col=q))

    ring(0, 1)

    with scope("psum"):
        landed(PPr.at[0 : N - 1], p1r)
        total = PPr[0].astype(F32)
        for p in range(1, N):
            total = total + PPr[p].astype(F32)
        PSb[...] = total.astype(BF16)
        PD[c] = PSb[...]
        to_col(lambda q: rcopy(PSb, PD.at[c], p2s, p2r, col=q))

    ring(2, 0)

    second_on(1)
    with scope("w_first2"):
        for h in range(2):
            first_landed(h, 2)
            first_landed(h, 3)
            second_out(h, 4, 2)

    ring(1, 1)
    ring(0, 2)

    second_on(2)
    second_on(3)

    ring(2, 1)

    with scope("p_on"):
        landed(PD.at[0 : N - 1], p2r)
        PE[r] = PD[r]
        to_row(lambda p: rcopy(PD.at[p], PE.at[r], pbs, pbr, row=p))

    ring(1, 2)
    second_on(4)
    ring(0, 3)
    ring(2, 2)

    with scope("w_end"):
        for h in range(2):
            for slot, j in offsets:
                second_landed(h, 2, slot, j)
                second_landed(h, 3, slot, j)
        landed(D1r.at[0 : N - 1], scr)
    for i in range(3):
        prepare(i)

    ring(1, 3)
    for i in range(3, L):
        prepare(i)
    ring(0, 4)
    ring_landed(0)
    grads_of(0)
    dots_of(0)
    ring(2, 3)
    grads_of(1)
    dots_of(1)

    with scope("u"):
        landed(PE.at[0 : N - 1], pbr)
        kind = lax.broadcasted_iota(jnp.int32, (256, 128), 0) % 16 // 2
        low = PE[...].reshape(N * 16, 256)
        inner_outer = jnp.zeros((256, 128), F32)
        for i in range(L):
            inner_outer = jnp.where(kind == i, nn(low, grads[i]), inner_outer)
        USb[:, 0:16, :] = inner_outer.astype(BF16).reshape(N, 16, 128)
        USr[r] = USb[r]
        to_row(lambda p: rcopy(USb.at[p], USr.at[r], uss, usr, row=p))

    ring(1, 4)
    ring_landed(1)
    dots_of(2)
    dots_of(3)
    grads_of(2)
    ring(2, 4)
    ring_landed(2)
    dots_of(4)
    dots_of(5)

    with scope("d1send"):
        D1r[c] = DL[:, own]
        to_col(lambda q: rcopy(DL.at[:, pl.ds(aligned(q, 128), 128)], D1r.at[c], d1s, d1r, col=q))
    for i in range(3, L):
        grads_of(i)
    stores = [
        pltpu.make_async_copy(o_in, h_in, out_s.at[0]),
        pltpu.make_async_copy(o_mag, h_mag_grad, out_s.at[1]),
        pltpu.make_async_copy(o_ain, h_ain_grad, out_s.at[2]),
        pltpu.make_async_copy(o_aout, h_aout_grad, out_s.at[3]),
    ]
    stores[0].start()
    with scope("irsend"):
        IRr[c] = IPf[c]
        to_col(lambda q: rcopy(IPf.at[q], IRr.at[c], irs, irr, col=q))

    with scope("d1"):
        landed(D1r.at[0 : N - 1], d1r)
        sub = D1r[0]
        for p in range(1, N):
            sub = sub + D1r[p]
        landed(SQr.at[0 : N - 1], scs)
        SQ[...] = sub
        D2r[r] = sub
        to_row(lambda p: rcopy(SQ, D2r.at[r], d2s, d2r, row=p))

    with scope("us"):
        landed(USr.at[0 : N - 1], usr)
        both = USr[0].astype(F32)
        for p in range(1, N):
            both = both + USr[p].astype(F32)

    with scope("d2"):
        landed(D2r.at[0 : N - 1], d2r)
        dots8 = D2r[0]
        for p in range(1, N):
            dots8 = dots8 + D2r[p]
        dots = dots8[0:L]
        o_mag[...] = dots / norms
        stores[1].start()
        correct = -mag[...] * dots / (norms * norms * norms)
        for i in range(L):
            CR[i : i + 1, own] = correct[i : i + 1]
        landed(D1r.at[0 : N - 1], d1s)
        landed(D2r.at[0 : N - 1], d2s)
        SQ[0:L] = correct
        to_col(lambda q: rcopy(SQ, CR.at[:, own], d3s, d3r, col=q))
        out = jnp.zeros((16, 128), F32)
        kind16 = lax.broadcasted_iota(jnp.int32, (16, 128), 0) // 2
        for i in range(L):
            out = jnp.where(kind16 == i, both[0:16] * scales[i : i + 1] + both[16:32] * correct[i : i + 1], out)
        OGr[r] = out
        to_row(lambda p: rcopy(OGr.at[r], OGr.at[r], ogs, ogr, row=p))

    with scope("ir"):
        landed(IRr.at[0 : N - 1], irr)
        in_sum = IRr[0]
        for p in range(1, N):
            in_sum = in_sum + IRr[p]
        IAr[c] = in_sum
        to_col(lambda q: rcopy(IAr.at[c], IAr.at[c], ias, iar, col=q))

    with scope("d3"):
        landed(D1r.at[0 : N - 1], d3r)
    with scope("term2"):
        for i in range(L):
            second_term = jnp.zeros((64, 128), F32)
            for n in range(NCH):
                cols = pl.ds(n * CH, CH)
                scaled_out = WA[i, 128:160, cols].astype(F32) * CR[i : i + 1, cols]
                high = scaled_out.astype(BF16)
                rest = (scaled_out - high.astype(F32)).astype(BF16)
                second_term += nt(jnp.concatenate([high, rest], axis=0), WM[i, :, cols])
            o_ain[i] = second_term[0:32] + second_term[32:64]

    with scope("og"):
        landed(OGr.at[0 : N - 1], ogr)
        out_all = OGr[...].reshape(N * 16, 128)
        for i in range(L):
            o_aout[i] = exact(collect(i), out_all)
        stores[3].start()

    with scope("ia"):
        landed(IAr.at[0 : N - 1], iar)
        in_all = IAr[...].reshape(N * 16, 128)
        for i in range(L):
            o_ain[i] += exact(collect(i), in_all)
        stores[2].start()

    with scope("drain"):
        for g in range(NG):
            landed(H.at[0 : N - 1, layers(g)], t1s.at[g])
            landed(H.at[0 : N - 1, layers(g)], t2s.at[g])
            for s in range(4):
                right(g, s).wait_send()
                left(g, s).wait_send()
            for n, i in enumerate(hops):
                over(g, n, i).wait_send()
        for h in range(2):
            for n, j in enumerate((0, 0, -1, 1)):
                first(h, n, j).wait_send()
            for slot, j in offsets:
                for n, jb in enumerate((0, 0, -1, 1)):
                    second(h, n, slot, j, jb).wait_send()
        landed(PPr.at[0 : N - 1], p1s)
        landed(USr.at[0 : N - 1], uss)
        landed(D1r.at[0 : N - 1], d3s)
        landed(OGr.at[0 : N - 1], ogs)
        landed(IRr.at[0 : N - 1], irs)
        landed(IAr.at[0 : N - 1], ias)

        landed(PPr.at[0 : N - 1], p2s)
        landed(PPr.at[0 : N - 1], pbs)
        for store in stores:
            store.wait()


def results(a, b, d, e, oa, ob, od, oe, sems):
    copies = [
        pltpu.make_async_copy(have, out, sems.at[n])
        for n, (have, out) in enumerate(((a, oa), (b, ob), (d, od), (e, oe)))
    ]
    for copy in copies:
        copy.start()
    for copy in copies:
        copy.wait()


def body(attn_out, out_cotangent, frozen, adapt_in, adapt_out, magnitude):
    dma = pltpu.SemaphoreType.DMA
    hbm = pl.BlockSpec(memory_space=pltpu.HBM)
    V = pltpu.VMEM
    scratch = [
        V((L, 256, 128), BF16),
        V((L, 256, 128), BF16),
        V((L, 32, 128), BF16),
        V((L, 128), F32),
        V((L, 256, 128), BF16),
        V((L, 32, 128), F32),
        V((L, 32, 128), F32),
        V((L, 128), F32),
        V((N, L, 16, 128), BF16),
        V((L, 256, 2048), BF16),
        V((L, 160, 2048), BF16),
        V((L, 128, 2048), F32),
        V((L, 128, 2048), BF16),
        V((8, 128), F32),
        V((N, 8, 128), F32),
        V((8, 2048), F32),
        V((8, 2048), F32),
        V((N, 16, 256), BF16),
        V((N, 16, 256), BF16),
        V((16, 256), BF16),
        V((N, 16, 256), BF16),
        V((N, 16, 256), BF16),
        V((N, 32, 128), BF16),
        V((N, 32, 128), BF16),
        V((8, 2048), F32),
        V((N, 8, 128), F32),
        V((N, 8, 128), F32),
        V((N, 16, 128), F32),
        V((N, 16, 128), F32),
        V((N, 16, 128), F32),
        V((N, 16, 128), F32),
        dma((6,)), dma((4,)),
        dma((NG,)), dma((NG,)), dma((NG,)), dma((NG,)),
        dma((NG, 4)), dma((NG, 4)), dma((NG, 4)), dma((NG, 4)),
        dma((NG, 8)), dma((NG, 8)),
        dma((2, 5, 4)), dma((2, 5, 4)),
        dma, dma, dma, dma, dma, dma, dma, dma,
        dma, dma, dma, dma,
        dma, dma, dma, dma, dma, dma, dma, dma, dma, dma, dma, dma,
    ]
    shapes = (
        jax.ShapeDtypeStruct((L, 256, 128), BF16),
        jax.ShapeDtypeStruct((L, 32, 128), F32),
        jax.ShapeDtypeStruct((L, 32, 128), F32),
        jax.ShapeDtypeStruct((L, 128), F32),
    )
    found = pl.pallas_call(
        kernel,
        out_shape=shapes,
        in_specs=[hbm] * 6,
        out_specs=(hbm,) * 4,
        scratch_shapes=scratch,
        compiler_params=pltpu.CompilerParams(
            collective_id=0, has_side_effects=True, vmem_limit_bytes=67043328
        ),
        name="dora",
    )(attn_out, out_cotangent, adapt_in, magnitude, frozen, adapt_out)
    return pl.pallas_call(
        results,
        out_shape=shapes,
        in_specs=[pl.BlockSpec(memory_space=pltpu.VMEM)] * 4,
        out_specs=(hbm,) * 4,
        scratch_shapes=[dma((4,))],
        compiler_params=pltpu.CompilerParams(vmem_limit_bytes=67043328),
        name="results",
    )(*found)

def solution(mesh):
    return jax.shard_map(
        body,
        mesh=mesh,
        in_specs=(
            P(None, "col", "row"),
            P(None, "row", "col"),
            P(None, "row", "col"),
            P(None, None, "row"),
            P(None, None, "col"),
            P(None, "col"),
        ),
        out_specs=(
            P(None, "col", "row"),
            P(None, None, "row"),
            P(None, None, "col"),
            P(None, "col"),
        ),
        check_vma=False,
    )
```

```python
import functools

import jax
import jax.numpy as jnp
from jax import lax
from jax.experimental import pallas as pl
from jax.experimental.pallas import tpu as pltpu
from jax.sharding import PartitionSpec as P

F32 = jnp.float32
BF16 = jnp.bfloat16
N = 16
ZS = 8
L = 6
NG = 3
GL = L // NG
CH = 512
NCH = 2048 // CH


def nn(a, b):
    return lax.dot_general(a, b, (((1,), (0,)), ((), ())), preferred_element_type=F32)


def nt(a, b):
    return lax.dot_general(a, b, (((1,), (1,)), ((), ())), preferred_element_type=F32)


def tn(a, b):
    return lax.dot_general(a, b, (((0,), (0,)), ((), ())), preferred_element_type=F32)


def aligned(i, n):
    return pl.multiple_of(i * n, n)


def kernel(
    h_acts, h_grads, h_ain, h_mag, h_frozen, h_aout,
    h_in, h_ain_grad, h_aout_grad, h_mag_grad,
    acts, grads, ain, mag, o_in, o_ain, o_aout, o_mag,
    H, G, WA, MF, WM, SQ, SQx, SQr, SC, CR, PPf, PPx, PPb, PPr, PSb, PD, PE, USb, USr, DL, D1r, D2r, OGr, IPf, IRr, IAr, TMP,
    in_s, out_s, t1s, t1r, t2s, t2r, rs, rr, ls, lr, ds, dr, ws, wr,
    sqs, sqr, scs, scr, p1s, p1r, p2s, p2r, pbs, pbr, uss, usr,
    d1s, d1r, d2s, d2r, d3s, d3r, ogs, ogr, irs, irr, ias, iar,
):
    r = lax.axis_index("row")
    c = lax.axis_index("col")
    z, k = r // 2, r % 2
    slot = k * ZS + z
    partner = z * 2 + 1 - k
    x, y = c // 4, c % 4
    scope = jax.named_scope

    def rcopy(src, dst, ss, rsem, **ids):
        return pltpu.make_async_remote_copy(
            src_ref=src, dst_ref=dst, send_sem=ss, recv_sem=rsem,
            device_id=ids, device_id_type=pl.DeviceIdType.MESH,
        )

    def landed(ref, sem):
        pltpu.make_async_copy(ref, ref, sem).wait()

    def to_row(make):
        def step(i, _):
            make(lax.rem(r + i, N)).start()
            return 0
        lax.fori_loop(1, N, step, 0)

    def to_col(make):
        def step(i, _):
            make(lax.rem(c + i, N)).start()
            return 0
        lax.fori_loop(1, N, step, 0)

    own = pl.ds(aligned(c, 128), 128)
    mine = pl.ds(aligned(r, 16), 16)

    def layers(g):
        return pl.ds(GL * g, GL)

    loads = [
        pltpu.make_async_copy(h_grads, grads, in_s.at[0]),
        pltpu.make_async_copy(h_frozen, WA.at[:, 0:128, own], in_s.at[1]),
        pltpu.make_async_copy(h_aout, WA.at[:, 128:160, own], in_s.at[2]),
        pltpu.make_async_copy(h_ain, ain, in_s.at[3]),
        pltpu.make_async_copy(h_acts, acts, in_s.at[4]),
        pltpu.make_async_copy(h_mag, mag, in_s.at[5]),
    ]
    with scope("s00_barrier"):
        barrier = pltpu.get_barrier_semaphore()

        def greet(i, _):
            pl.semaphore_signal(barrier, inc=1, device_id={"row": lax.rem(r + i, N)}, device_id_type=pl.DeviceIdType.MESH)
            pl.semaphore_signal(barrier, inc=1, device_id={"col": lax.rem(c + i, N)}, device_id_type=pl.DeviceIdType.MESH)
            return 0

        lax.fori_loop(1, N, greet, 0)
        for load in loads:
            load.start()
        for load in loads:
            load.wait()
        H[r] = grads[:, mine, :]
        pl.semaphore_wait(barrier, 2 * (N - 1))

    with scope("s01_t1send"):
        for g in range(NG):
            to_row(lambda p, g=g: rcopy(
                grads.at[layers(g), pl.ds(aligned(p, 16), 16), :], H.at[r, layers(g)],
                t1s.at[g], t1r.at[g], row=p))

    def place_of(h, a, b):
        return 4 * b + a if h == 0 else 4 * a + b

    pos = ((y, x), (x, y))
    cuts = ((0, 160), (0, 160), (0, 80), (80, 160))

    def wblock(h, a, b, lo=0, hi=160):
        return WA.at[pl.ds(3 * h, 3), lo:hi, pl.ds(aligned(place_of(h, a, b), 128), 128)]

    def mod4(i):
        return lax.rem(i + 4, 4)

    def w_copy(h, kind, slot, a, b, target):
        ref = wblock(h, a, b, *cuts[kind])
        return rcopy(ref, ref, ws.at[h, slot, kind], wr.at[h, slot, kind], col=target)

    def first(h, kind, j):
        a, b = pos[h]
        step = 1 if kind in (0, 2) else -1
        return w_copy(h, kind, 0, mod4(a + j), b, place_of(h, mod4(a + step), b))

    def second(h, kind, slot, j, jb):
        a, b = pos[h]
        step = 1 if kind in (0, 2) else -1
        return w_copy(h, kind, slot, mod4(a + j), mod4(b + jb), place_of(h, a, mod4(b + step)))

    def first_landed(h, kind):
        a, b = pos[h]
        landed(wblock(h, mod4(a + (-1, 1, 2, 2)[kind]), b, *cuts[kind]), wr.at[h, 0, kind])

    def second_landed(h, kind, slot, j):
        a, b = pos[h]
        landed(wblock(h, mod4(a + j), mod4(b + (-1, 1, 2, 2)[kind]), *cuts[kind]), wr.at[h, slot, kind])

    offsets = ((1, 0), (2, -1), (3, 1), (4, 2))

    def second_out(h, slot, j):
        second(h, 0, slot, j, 0).start()
        second(h, 1, slot, j, 0).start()

    def second_on(slot):
        with scope(f"w_on{slot}"):
            j = dict(offsets)[slot]
            for h in range(2):
                second_landed(h, 0, slot, j)
                second(h, 2, slot, j, -1).start()
                second_landed(h, 1, slot, j)
                second(h, 3, slot, j, 1).start()

    for h in range(2):
        first(h, 0, 0).start()
        first(h, 1, 0).start()
    for h in range(2):
        second_out(h, 1, 0)

    rows = lax.broadcasted_iota(jnp.int32, (256, 32), 0)
    ranks = lax.broadcasted_iota(jnp.int32, (256, 32), 1)

    def spread(i):
        off = rows % 16 - 2 * i
        return jnp.where((off >= 0) & (off < 2) & (ranks == rows // 16 * 2 + off), 1.0, 0.0).astype(F32)

    with scope("s02_local"):
        SQ[...] = jnp.zeros((8, 128), F32)
        part = jnp.zeros((256, 256), F32)
        inner = jnp.zeros((256, 128), F32)
        for i in range(L):
            block = WA[i, 0:128, own].astype(F32) + tn(ain[i], WA[i, 128:160, own])
            SQ[i : i + 1] = jnp.sum(block * block, axis=0, keepdims=True)
            wide = nn(spread(i).astype(BF16), ain[i]).astype(BF16)
            part += nt(wide, acts[i])
            high = block.astype(BF16)
            inner += nn(wide, high) + nn(wide, (block - high.astype(F32)).astype(BF16))
        PPf[...] = part.reshape(N, 16, 256)
        USb[:, 16:32, :] = inner.astype(BF16).reshape(N, 16, 128)
        theirs = pl.ds(aligned(1 - k, ZS), ZS)
        to_partner = [
            rcopy(SQ, SQx, sqs, sqr.at[0], row=partner),
            rcopy(PPf.at[theirs], PPx, p1s, p1r.at[0], row=partner),
        ]
        for copy in to_partner:
            copy.start()

    def to_column(make):
        def step(i, _):
            make(lax.rem(z + i, ZS)).start()
            return 0
        lax.fori_loop(1, ZS, step, 0)

    with scope("pairs"):
        for copy in to_partner:
            copy.wait()
        SQ[...] = SQ[...] + SQx[...]
        SQr[z] = SQ[...]
        to_column(lambda q: rcopy(SQ, SQr.at[z], sqs, sqr.at[1], row=q * 2 + k))
        PPb[...] = (PPf[pl.ds(aligned(k, ZS), ZS)] + PPx[...]).astype(BF16)
        PPr[z] = PPb[z]
        to_column(lambda q: rcopy(PPb.at[q], PPr.at[z], p1s, p1r.at[1], row=q * 2 + k))

    def exchange(g):
        with scope(f"t2_{g}"):
            landed(H.at[0 : N - 1, layers(g)], t1r.at[g])
            to_col(lambda q: rcopy(
                H.at[q, layers(g)], G.at[layers(g), mine, own], t2s.at[g], t2r.at[g], col=q))
            G[GL * g : GL * g + GL, mine, own] = H[c, GL * g : GL * g + GL]

    def chunk(g, q, count=GL, at=0):
        return G.at[pl.ds(GL * g + at, count), pl.ds(aligned(q, 16), 16), :]

    def across(i):
        return lax.rem(z + i + ZS, ZS) * 2 + k

    def right(g, s):
        ref = chunk(g, across(-s)) if s < 3 else chunk(g, across(-s), 1, 0)
        return rcopy(ref, ref, rs.at[g, s], rr.at[g, s], row=across(1))

    def left(g, s):
        ref = chunk(g, across(s)) if s < 3 else chunk(g, across(s), 1, 1)
        return rcopy(ref, ref, ls.at[g, s], lr.at[g, s], row=across(-1))

    def over(g, n, i):
        ref = chunk(g, across(i))
        return rcopy(ref, ref, ds.at[g, n], dr.at[g, n], row=partner)

    hops = (0, -1, -2, -3, 1, 2, 3, 4)

    def ring(g, s):
        with scope(f"r{g}{s}"):
            if s == 0:
                landed(G.at[layers(g), mine, 0 : 128 * (N - 1)], t2r.at[g])
                right(g, 0).start()
                left(g, 0).start()
                over(g, 0, 0).start()
            elif s < 4:
                landed(chunk(g, across(-s)), rr.at[g, s - 1])
                right(g, s).start()
                landed(chunk(g, across(s)), lr.at[g, s - 1])
                left(g, s).start()
                over(g, s, -s).start()
                over(g, 3 + s, s).start()
            else:
                landed(chunk(g, across(4), 1, 0), rr.at[g, 3])
                landed(chunk(g, across(4), 1, 1), lr.at[g, 3])
                over(g, 7, 4).start()

    def ring_landed(g):
        with scope(f"r{g}_landed"):
            for n, i in enumerate(hops):
                landed(chunk(g, lax.rem(z + i + ZS, ZS) * 2 + 1 - k), dr.at[g, n])

    def prepare(i):
        with scope(f"prep{i}"):
            for n in range(NCH):
                cols = pl.ds(n * CH, CH)
                merged = WA[i, 0:128, cols].astype(F32) + tn(ain[i], WA[i, 128:160, cols])
                MF[i, :, cols] = merged
                WM[i, :, cols] = merged.astype(BF16)

    def dots_of(i):
        with scope(f"dots{i}"):
            for n in range(NCH):
                cols = pl.ds(n * CH, CH)
                outer = tn(acts[i], G[i, :, cols])
                DL[i : i + 1, cols] = jnp.sum(MF[i, :, cols] * outer, axis=0, keepdims=True)

    def grads_of(i):
        with scope(f"grads{i}"):
            got = jnp.zeros((256, 128), F32)
            low_t = jnp.zeros((32, 256), F32)
            for n in range(NCH):
                cols = pl.ds(n * CH, CH)
                scaled = (G[i, :, cols].astype(F32) * SC[i : i + 1, cols]).astype(BF16)
                got += nt(scaled, WM[i, :, cols])
                low_t += nt(WA[i, 128:160, cols], scaled)
            o_in[i] = got.astype(BF16)
            high = low_t.astype(BF16)
            rest = (low_t - high.astype(F32)).astype(BF16)
            TMP[...] = nn(high, acts[i]) + nn(rest, acts[i])
            for q in range(2):
                IPf[pl.ds(2 * i + q, N, stride=16), :] = TMP[pl.ds(q, N, stride=2), :]

    DL[...] = jnp.zeros((8, 2048), F32)
    IPf[...] = jnp.zeros((N * 16, 128), F32)

    exchange(0)
    exchange(1)

    with scope("w_first"):
        for h in range(2):
            first_landed(h, 0)
            first(h, 2, -1).start()
            first_landed(h, 1)
            first(h, 3, 1).start()

    ring(0, 0)
    exchange(2)
    for h in range(2):
        second_out(h, 2, -1)
        second_out(h, 3, 1)
    second_on(1)
    ring(1, 0)

    with scope("norms"):
        landed(SQr.at[0 : ZS - 1], sqr.at[1])
        squares = SQr[0]
        for p in range(1, ZS):
            squares = squares + SQr[p]
        norms = jnp.sqrt(squares[0:L] + 0.25)
        scales = mag[...] / norms
        for i in range(L):
            SC[i : i + 1, own] = scales[i : i + 1]
        landed(SQr.at[0 : ZS - 1], sqs)
        SQ[0:L] = scales
        to_col(lambda q: rcopy(SQ, SC.at[:, own], scs, scr, col=q))

    ring(0, 1)

    with scope("psum"):
        landed(PPr.at[0 : ZS - 1], p1r.at[1])
        total = PPr[0].astype(F32)
        for p in range(1, ZS):
            total = total + PPr[p].astype(F32)
        PSb[...] = total.astype(BF16)
        PD[c] = PSb[...]
        to_col(lambda q: rcopy(PSb, PD.at[c], p2s, p2r, col=q))

    ring(2, 0)

    with scope("w_first2"):
        for h in range(2):
            first_landed(h, 2)
            first_landed(h, 3)
            second_out(h, 4, 2)

    ring(1, 1)
    second_on(2)
    second_on(3)
    ring(2, 1)
    ring(0, 2)
    ring(1, 2)
    second_on(4)
    ring(2, 2)

    with scope("w_end"):
        for h in range(2):
            for place, j in offsets:
                second_landed(h, 2, place, j)
                second_landed(h, 3, place, j)
        landed(D1r.at[0 : N - 1], scr)
    for i in range(3):
        prepare(i)

    ring(0, 3)
    for i in range(3, L):
        prepare(i)
    ring(1, 3)
    ring(2, 3)

    with scope("p_on"):
        landed(PD.at[0 : N - 1], p2r)
        PE[slot] = PD[r]
        to_row(lambda p: rcopy(PD.at[p], PE.at[slot], pbs, pbr, row=p))

    ring(0, 4)
    ring(1, 4)
    ring_landed(0)
    dots_of(0)
    dots_of(1)
    ring(2, 4)
    ring_landed(1)
    dots_of(2)
    dots_of(3)
    ring_landed(2)
    dots_of(4)
    dots_of(5)

    with scope("d1send"):
        D1r[c] = DL[:, own]
        to_col(lambda q: rcopy(DL.at[:, pl.ds(aligned(q, 128), 128)], D1r.at[c], d1s, d1r, col=q))
    with scope("u"):
        landed(PE.at[0 : N - 1], pbr)
        kind = lax.broadcasted_iota(jnp.int32, (256, 128), 0) % 16 // 2
        low = PE[...].reshape(N * 16, 256)
        inner_outer = jnp.zeros((256, 128), F32)
        for i in range(L):
            inner_outer = jnp.where(kind == i, nn(low, grads[i]), inner_outer)
        USb[:, 0:16, :] = inner_outer.astype(BF16).reshape(N, 16, 128)
        USr[slot] = USb[slot]
        to_row(lambda p: rcopy(USb.at[lax.rem(p, 2) * ZS + p // 2], USr.at[slot], uss, usr, row=p))

    for i in range(4):
        grads_of(i)

    with scope("d1"):
        landed(D1r.at[0 : N - 1], d1r)
        sub = D1r[0]
        for p in range(1, N):
            sub = sub + D1r[p]
        landed(D1r.at[0 : N - 1], scs)
        SQ[...] = sub
        D2r[r] = sub
        to_row(lambda p: rcopy(SQ, D2r.at[r], d2s, d2r, row=p))

    for i in range(4, L):
        grads_of(i)
    stores = [
        pltpu.make_async_copy(o_in, h_in, out_s.at[0]),
        pltpu.make_async_copy(o_mag, h_mag_grad, out_s.at[1]),
        pltpu.make_async_copy(o_ain, h_ain_grad, out_s.at[2]),
        pltpu.make_async_copy(o_aout, h_aout_grad, out_s.at[3]),
    ]
    stores[0].start()
    with scope("irsend"):
        IRr[c] = IPf[pl.ds(aligned(c, 16), 16), :]
        to_col(lambda q: rcopy(IPf.at[pl.ds(aligned(q, 16), 16), :], IRr.at[c], irs, irr, col=q))

    with scope("drain0"):
        for g in range(NG):
            landed(H.at[0 : N - 1, layers(g)], t1s.at[g])
            landed(H.at[0 : N - 1, layers(g)], t2s.at[g])
            for s in range(4):
                right(g, s).wait_send()
                left(g, s).wait_send()
            for n, i in enumerate(hops):
                over(g, n, i).wait_send()
        for h in range(2):
            for n, j in enumerate((0, 0, -1, 1)):
                first(h, n, j).wait_send()
            for place, j in offsets:
                for n, jb in enumerate((0, 0, -1, 1)):
                    second(h, n, place, j, jb).wait_send()
        landed(PPr.at[0 : ZS - 1], p1s)
        landed(PD.at[0 : N - 1], p2s)
        landed(PD.at[0 : N - 1], pbs)

    with scope("us"):
        landed(USr.at[0 : N - 1], usr)
        both = USr[0].astype(F32)
        for p in range(1, N):
            both = both + USr[p].astype(F32)

    with scope("d2"):
        landed(D2r.at[0 : N - 1], d2r)
        dots8 = D2r[0]
        for p in range(1, N):
            dots8 = dots8 + D2r[p]
        dots = dots8[0:L]
        o_mag[...] = dots / norms
        stores[1].start()
        correct = -mag[...] * dots / (norms * norms * norms)
        for i in range(L):
            CR[i : i + 1, own] = correct[i : i + 1]
        landed(D1r.at[0 : N - 1], d1s)
        landed(D2r.at[0 : N - 1], d2s)
        SQ[0:L] = correct
        to_col(lambda q: rcopy(SQ, CR.at[:, own], d3s, d3r, col=q))
        out = jnp.zeros((16, 128), F32)
        kind16 = lax.broadcasted_iota(jnp.int32, (16, 128), 0) // 2
        for i in range(L):
            out = jnp.where(kind16 == i, both[0:16] * scales[i : i + 1] + both[16:32] * correct[i : i + 1], out)
        OGr[pl.ds(aligned(slot, 16), 16), :] = out
        ranks_out = OGr.at[pl.ds(aligned(slot, 16), 16), :]
        to_row(lambda p: rcopy(ranks_out, ranks_out, ogs, ogr, row=p))

    with scope("ir"):
        landed(IRr.at[0 : N - 1], irr)
        in_sum = IRr[0]
        for p in range(1, N):
            in_sum = in_sum + IRr[p]
        IAr[pl.ds(aligned(c, 16), 16), :] = in_sum
        block = IAr.at[pl.ds(aligned(c, 16), 16), :]
        to_col(lambda q: rcopy(block, block, ias, iar, col=q))

    with scope("d3"):
        landed(D1r.at[0 : N - 1], d3r)
    with scope("term2"):
        for i in range(L):
            second_term = jnp.zeros((128, 64), F32)
            for n in range(NCH):
                cols = pl.ds(n * CH, CH)
                scaled_out = WA[i, 128:160, cols].astype(F32) * CR[i : i + 1, cols]
                high = scaled_out.astype(BF16)
                rest = (scaled_out - high.astype(F32)).astype(BF16)
                second_term += nt(WM[i, :, cols], jnp.concatenate([high, rest], axis=0))
            o_ain[i] = jnp.transpose(second_term[:, 0:32] + second_term[:, 32:64])

    with scope("og"):
        landed(OGr.at[0 : 240, :], ogr)
        for i in range(L):
            for q in range(2):
                o_aout[i, pl.ds(q, N, stride=2), :] = OGr[pl.ds(2 * i + q, N, stride=16), :]
        stores[3].start()

    with scope("ia"):
        landed(IAr.at[0 : 240, :], iar)
        for i in range(L):
            for q in range(2):
                o_ain[i, pl.ds(q, N, stride=2), :] += IAr[pl.ds(2 * i + q, N, stride=16), :]
        stores[2].start()

    with scope("drain"):
        landed(USr.at[0 : N - 1], uss)
        landed(D1r.at[0 : N - 1], d3s)
        landed(OGr.at[0 : 240, :], ogs)
        landed(IRr.at[0 : N - 1], irs)
        landed(IAr.at[0 : 240, :], ias)
        for store in stores:
            store.wait()


def results(a, b, d, e, oa, ob, od, oe, va, vb, vd, ve, sems):
    into = []
    away = []
    for n, (have, held, out) in enumerate(((a, va, oa), (b, vb, ob), (d, vd, od), (e, ve, oe))):
        into.append(pltpu.make_async_copy(have, held, sems.at[n]))
        away.append(pltpu.make_async_copy(held, out, sems.at[4 + n]))
    for copy in into:
        copy.start()
    for n in range(4):
        into[n].wait()
        away[n].start()
    for copy in away:
        copy.wait()


def body(attn_out, out_cotangent, frozen, adapt_in, adapt_out, magnitude):
    dma = pltpu.SemaphoreType.DMA
    hbm = pl.BlockSpec(memory_space=pltpu.HBM)
    V = pltpu.VMEM
    scratch = [
        V((L, 256, 128), BF16),
        V((L, 256, 128), BF16),
        V((L, 32, 128), BF16),
        V((L, 128), F32),
        V((L, 256, 128), BF16),
        V((L, 32, 128), F32),
        V((L, 32, 128), F32),
        V((L, 128), F32),
        V((N, L, 16, 128), BF16),
        V((L, 256, 2048), BF16),
        V((L, 160, 2048), BF16),
        V((L, 128, 2048), F32),
        V((L, 128, 2048), BF16),
        V((8, 128), F32),
        V((8, 128), F32),
        V((ZS, 8, 128), F32),
        V((8, 2048), F32),
        V((8, 2048), F32),
        V((N, 16, 256), F32),
        V((ZS, 16, 256), F32),
        V((ZS, 16, 256), BF16),
        V((ZS, 16, 256), BF16),
        V((16, 256), BF16),
        V((N, 16, 256), BF16),
        V((N, 16, 256), BF16),
        V((N, 32, 128), BF16),
        V((N, 32, 128), BF16),
        V((8, 2048), F32),
        V((N, 8, 128), F32),
        V((N, 8, 128), F32),
        V((N * 16, 128), F32),
        V((N * 16, 128), F32),
        V((N, 16, 128), F32),
        V((N * 16, 128), F32),
        V((32, 128), F32),
        dma((6,)), dma((4,)),
        dma((NG,)), dma((NG,)), dma((NG,)), dma((NG,)),
        dma((NG, 4)), dma((NG, 4)), dma((NG, 4)), dma((NG, 4)),
        dma((NG, 8)), dma((NG, 8)),
        dma((2, 5, 4)), dma((2, 5, 4)),
        dma, dma((2,)), dma, dma, dma, dma((2,)), dma, dma,
        dma, dma, dma, dma,
        dma, dma, dma, dma, dma, dma, dma, dma, dma, dma, dma, dma,
    ]
    shapes = (
        jax.ShapeDtypeStruct((L, 256, 128), BF16),
        jax.ShapeDtypeStruct((L, 32, 128), F32),
        jax.ShapeDtypeStruct((L, 32, 128), F32),
        jax.ShapeDtypeStruct((L, 128), F32),
    )
    found = pl.pallas_call(
        kernel,
        out_shape=shapes,
        in_specs=[hbm] * 6,
        out_specs=(hbm,) * 4,
        scratch_shapes=scratch,
        compiler_params=pltpu.CompilerParams(
            collective_id=0, has_side_effects=True, vmem_limit_bytes=67043328
        ),
        name="dora",
    )(attn_out, out_cotangent, adapt_in, magnitude, frozen, adapt_out)
    return pl.pallas_call(
        results,
        out_shape=shapes,
        in_specs=[hbm] * 4,
        out_specs=(hbm,) * 4,
        scratch_shapes=[V(shape.shape, shape.dtype) for shape in shapes] + [dma((8,))],
        compiler_params=pltpu.CompilerParams(vmem_limit_bytes=67043328),
        name="results",
    )(*found)

def solution(mesh):
    return jax.shard_map(
        body,
        mesh=mesh,
        in_specs=(
            P(None, "col", "row"),
            P(None, "row", "col"),
            P(None, "row", "col"),
            P(None, None, "row"),
            P(None, None, "col"),
            P(None, "col"),
        ),
        out_specs=(
            P(None, "col", "row"),
            P(None, None, "row"),
            P(None, None, "col"),
            P(None, "col"),
        ),
        check_vma=False,
    )
```

```python
import functools

import jax
import jax.numpy as jnp
from jax import lax
from jax.experimental import pallas as pl
from jax.experimental.pallas import tpu as pltpu
from jax.sharding import PartitionSpec as P

F32 = jnp.float32
BF16 = jnp.bfloat16
N = 16
ZS = 8
L = 6
NG = 3
GL = L // NG
CH = 512
NCH = 2048 // CH


def nn(a, b):
    return lax.dot_general(a, b, (((1,), (0,)), ((), ())), preferred_element_type=F32)


def nt(a, b):
    return lax.dot_general(a, b, (((1,), (1,)), ((), ())), preferred_element_type=F32)


def tn(a, b):
    return lax.dot_general(a, b, (((0,), (0,)), ((), ())), preferred_element_type=F32)


def aligned(i, n):
    return pl.multiple_of(i * n, n)


def kernel(
    h_acts, h_grads, h_ain, h_mag, h_frozen, h_aout,
    h_in, h_ain_grad, h_aout_grad, h_mag_grad,
    acts, grads, ain, mag, o_in, o_ain, o_aout, o_mag,
    H, G, WA, MF, WM, SQ, SQx, SQr, SC, CR, PPf, PPx, PPb, PPr, PSb, PD, PE, USb, USr, DL, D1r, D2r, OGr, IPf, IRr, IAr, TMP,
    in_s, out_s, t1s, t1r, t2s, t2r, rs, rr, ls, lr, ds, dr, ws, wr,
    sqs, sqr, scs, scr, p1s, p1r, p2s, p2r, pbs, pbr, uss, usr,
    d1s, d1r, d2s, d2r, d3s, d3r, ogs, ogr, irs, irr, ias, iar,
):
    r = lax.axis_index("row")
    c = lax.axis_index("col")
    z, k = r // 2, r % 2
    slot = k * ZS + z
    partner = z * 2 + 1 - k
    x, y = c // 4, c % 4
    scope = jax.named_scope

    def rcopy(src, dst, ss, rsem, **ids):
        return pltpu.make_async_remote_copy(
            src_ref=src, dst_ref=dst, send_sem=ss, recv_sem=rsem,
            device_id=ids, device_id_type=pl.DeviceIdType.MESH,
        )

    def landed(ref, sem):
        pltpu.make_async_copy(ref, ref, sem).wait()

    def to_row(make):
        def step(i, _):
            make(lax.rem(r + i, N)).start()
            return 0
        lax.fori_loop(1, N, step, 0)

    def to_col(make):
        def step(i, _):
            make(lax.rem(c + i, N)).start()
            return 0
        lax.fori_loop(1, N, step, 0)

    def quick_row(make):
        for i in (8, 7, 9, 6, 10, 5, 11, 4, 12, 3, 13, 2, 14, 1, 15):
            make(lax.rem(r + i, N)).start()

    def quick_col(make):
        for i in (10, 9, 11, 6, 14, 8, 2, 5, 7, 13, 15, 4, 12, 1, 3):
            make(lax.rem(x + i // 4, 4) * 4 + lax.rem(y + i % 4, 4)).start()

    own = pl.ds(aligned(c, 128), 128)
    mine = pl.ds(aligned(r, 16), 16)

    def layers(g):
        return pl.ds(GL * g, GL)

    loads = [
        pltpu.make_async_copy(h_grads, grads, in_s.at[0]),
        pltpu.make_async_copy(h_frozen, WA.at[:, 0:128, own], in_s.at[1]),
        pltpu.make_async_copy(h_aout, WA.at[:, 128:160, own], in_s.at[2]),
        pltpu.make_async_copy(h_ain, ain, in_s.at[3]),
        pltpu.make_async_copy(h_acts, acts, in_s.at[4]),
        pltpu.make_async_copy(h_mag, mag, in_s.at[5]),
    ]
    with scope("s00_barrier"):
        barrier = pltpu.get_barrier_semaphore()

        def greet(i, _):
            pl.semaphore_signal(barrier, inc=1, device_id={"row": lax.rem(r + i, N)}, device_id_type=pl.DeviceIdType.MESH)
            pl.semaphore_signal(barrier, inc=1, device_id={"col": lax.rem(c + i, N)}, device_id_type=pl.DeviceIdType.MESH)
            return 0

        lax.fori_loop(1, N, greet, 0)
        for load in loads:
            load.start()
        for load in loads:
            load.wait()
        H[r] = grads[:, mine, :]
        pl.semaphore_wait(barrier, 2 * (N - 1))

    with scope("s01_t1send"):
        for g in range(NG):
            to_row(lambda p, g=g: rcopy(
                grads.at[layers(g), pl.ds(aligned(p, 16), 16), :], H.at[r, layers(g)],
                t1s.at[g], t1r.at[g], row=p))

    def place_of(h, a, b):
        return 4 * b + a if h == 0 else 4 * a + b

    pos = ((y, x), (x, y))
    cuts = ((0, 160), (0, 160), (0, 80), (80, 160))

    def wblock(h, a, b, lo=0, hi=160):
        return WA.at[pl.ds(3 * h, 3), lo:hi, pl.ds(aligned(place_of(h, a, b), 128), 128)]

    def mod4(i):
        return lax.rem(i + 4, 4)

    def w_copy(h, kind, slot, a, b, target):
        ref = wblock(h, a, b, *cuts[kind])
        return rcopy(ref, ref, ws.at[h, slot, kind], wr.at[h, slot, kind], col=target)

    def first(h, kind, j):
        a, b = pos[h]
        step = 1 if kind in (0, 2) else -1
        return w_copy(h, kind, 0, mod4(a + j), b, place_of(h, mod4(a + step), b))

    def second(h, kind, slot, j, jb):
        a, b = pos[h]
        step = 1 if kind in (0, 2) else -1
        return w_copy(h, kind, slot, mod4(a + j), mod4(b + jb), place_of(h, a, mod4(b + step)))

    def first_landed(h, kind):
        a, b = pos[h]
        landed(wblock(h, mod4(a + (-1, 1, 2, 2)[kind]), b, *cuts[kind]), wr.at[h, 0, kind])

    def second_landed(h, kind, slot, j):
        a, b = pos[h]
        landed(wblock(h, mod4(a + j), mod4(b + (-1, 1, 2, 2)[kind]), *cuts[kind]), wr.at[h, slot, kind])

    offsets = ((1, 0), (2, -1), (3, 1), (4, 2))

    def second_out(h, slot, j):
        second(h, 0, slot, j, 0).start()
        second(h, 1, slot, j, 0).start()

    def second_on(slot):
        with scope(f"w_on{slot}"):
            j = dict(offsets)[slot]
            for h in range(2):
                second_landed(h, 0, slot, j)
                second(h, 2, slot, j, -1).start()
                second_landed(h, 1, slot, j)
                second(h, 3, slot, j, 1).start()

    for h in range(2):
        first(h, 0, 0).start()
        first(h, 1, 0).start()
    for h in range(2):
        second_out(h, 1, 0)

    rows = lax.broadcasted_iota(jnp.int32, (256, 32), 0)
    ranks = lax.broadcasted_iota(jnp.int32, (256, 32), 1)

    def spread(i):
        off = rows % 16 - 2 * i
        return jnp.where((off >= 0) & (off < 2) & (ranks == rows // 16 * 2 + off), 1.0, 0.0).astype(F32)

    with scope("s02_local"):
        SQ[...] = jnp.zeros((8, 128), F32)
        part = jnp.zeros((256, 256), F32)
        inner = jnp.zeros((256, 128), F32)
        for i in range(L):
            block = WA[i, 0:128, own].astype(F32) + tn(ain[i], WA[i, 128:160, own])
            SQ[i : i + 1] = jnp.sum(block * block, axis=0, keepdims=True)
            wide = nn(spread(i).astype(BF16), ain[i]).astype(BF16)
            part += nt(wide, acts[i])
            high = block.astype(BF16)
            inner += nn(wide, high) + nn(wide, (block - high.astype(F32)).astype(BF16))
        PPf[...] = part.reshape(N, 16, 256)
        USb[:, 16:32, :] = inner.astype(BF16).reshape(N, 16, 128)
        theirs = pl.ds(aligned(1 - k, ZS), ZS)
        to_partner = [
            rcopy(SQ, SQx, sqs, sqr.at[0], row=partner),
            rcopy(PPf.at[theirs], PPx, p1s, p1r.at[0], row=partner),
        ]
        for copy in to_partner:
            copy.start()

    def to_column(make):
        def step(i, _):
            make(lax.rem(z + i, ZS)).start()
            return 0
        lax.fori_loop(1, ZS, step, 0)

    with scope("pairs"):
        for copy in to_partner:
            copy.wait()
        SQ[...] = SQ[...] + SQx[...]
        SQr[z] = SQ[...]
        to_column(lambda q: rcopy(SQ, SQr.at[z], sqs, sqr.at[1], row=q * 2 + k))
        PPb[...] = (PPf[pl.ds(aligned(k, ZS), ZS)] + PPx[...]).astype(BF16)
        PPr[z] = PPb[z]
        to_column(lambda q: rcopy(PPb.at[q], PPr.at[z], p1s, p1r.at[1], row=q * 2 + k))

    def exchange(g):
        with scope(f"t2_{g}"):
            landed(H.at[0 : N - 1, layers(g)], t1r.at[g])
            to_col(lambda q: rcopy(
                H.at[q, layers(g)], G.at[layers(g), mine, own], t2s.at[g], t2r.at[g], col=q))
            G[GL * g : GL * g + GL, mine, own] = H[c, GL * g : GL * g + GL]

    def chunk(g, q, count=GL, at=0):
        return G.at[pl.ds(GL * g + at, count), pl.ds(aligned(q, 16), 16), :]

    def across(i):
        return lax.rem(z + i + ZS, ZS) * 2 + k

    def right(g, s):
        ref = chunk(g, across(-s)) if s < 3 else chunk(g, across(-s), 1, 0)
        return rcopy(ref, ref, rs.at[g, s], rr.at[g, s], row=across(1))

    def left(g, s):
        ref = chunk(g, across(s)) if s < 3 else chunk(g, across(s), 1, 1)
        return rcopy(ref, ref, ls.at[g, s], lr.at[g, s], row=across(-1))

    def over(g, n, i):
        ref = chunk(g, across(i))
        return rcopy(ref, ref, ds.at[g, n], dr.at[g, n], row=partner)

    hops = (0, -1, -2, -3, 1, 2, 3, 4)

    def ring(g, s):
        with scope(f"r{g}{s}"):
            if s == 0:
                landed(G.at[layers(g), mine, 0 : 128 * (N - 1)], t2r.at[g])
                right(g, 0).start()
                left(g, 0).start()
                over(g, 0, 0).start()
            elif s < 4:
                landed(chunk(g, across(-s)), rr.at[g, s - 1])
                right(g, s).start()
                landed(chunk(g, across(s)), lr.at[g, s - 1])
                left(g, s).start()
                over(g, s, -s).start()
                over(g, 3 + s, s).start()
            else:
                landed(chunk(g, across(4), 1, 0), rr.at[g, 3])
                landed(chunk(g, across(4), 1, 1), lr.at[g, 3])
                over(g, 7, 4).start()

    def ring_landed(g):
        with scope(f"r{g}_landed"):
            for n, i in enumerate(hops):
                landed(chunk(g, lax.rem(z + i + ZS, ZS) * 2 + 1 - k), dr.at[g, n])

    def prepare(i):
        with scope(f"prep{i}"):
            for n in range(NCH):
                cols = pl.ds(n * CH, CH)
                merged = WA[i, 0:128, cols].astype(F32) + tn(ain[i], WA[i, 128:160, cols])
                MF[i, :, cols] = merged
                WM[i, :, cols] = merged.astype(BF16)

    def dots_of(i):
        with scope(f"dots{i}"):
            for n in range(NCH):
                cols = pl.ds(n * CH, CH)
                outer = tn(acts[i], G[i, :, cols])
                DL[i : i + 1, cols] = jnp.sum(MF[i, :, cols] * outer, axis=0, keepdims=True)

    def grads_of(i):
        with scope(f"grads{i}"):
            got = jnp.zeros((256, 128), F32)
            low_t = jnp.zeros((32, 256), F32)
            for n in range(NCH):
                cols = pl.ds(n * CH, CH)
                scaled = (G[i, :, cols].astype(F32) * SC[i : i + 1, cols]).astype(BF16)
                got += nt(scaled, WM[i, :, cols])
                low_t += nt(WA[i, 128:160, cols], scaled)
            o_in[i] = got.astype(BF16)
            high = low_t.astype(BF16)
            rest = (low_t - high.astype(F32)).astype(BF16)
            TMP[...] = nn(high, acts[i]) + nn(rest, acts[i])
            for q in range(2):
                IPf[pl.ds(2 * i + q, N, stride=16), :] = TMP[pl.ds(q, N, stride=2), :]

    DL[...] = jnp.zeros((8, 2048), F32)
    IPf[...] = jnp.zeros((N * 16, 128), F32)

    exchange(0)
    exchange(1)

    with scope("w_first"):
        for h in range(2):
            first_landed(h, 0)
            first(h, 2, -1).start()
            first_landed(h, 1)
            first(h, 3, 1).start()

    ring(0, 0)
    exchange(2)
    for h in range(2):
        second_out(h, 2, -1)
        second_out(h, 3, 1)
    second_on(1)
    ring(1, 0)

    with scope("norms"):
        landed(SQr.at[0 : ZS - 1], sqr.at[1])
        squares = SQr[0]
        for p in range(1, ZS):
            squares = squares + SQr[p]
        norms = jnp.sqrt(squares[0:L] + 0.25)
        scales = mag[...] / norms
        minus = -mag[...] / (norms * norms * norms)
        for i in range(L):
            SC[i : i + 1, own] = scales[i : i + 1]
        landed(SQr.at[0 : ZS - 1], sqs)
        SQ[0:L] = scales
        to_col(lambda q: rcopy(SQ, SC.at[:, own], scs, scr, col=q))

    ring(0, 1)

    with scope("psum"):
        landed(PPr.at[0 : ZS - 1], p1r.at[1])
        total = PPr[0].astype(F32)
        for p in range(1, ZS):
            total = total + PPr[p].astype(F32)
        PSb[...] = total.astype(BF16)
        PD[c] = PSb[...]
        to_col(lambda q: rcopy(PSb, PD.at[c], p2s, p2r, col=q))

    ring(2, 0)

    with scope("w_first2"):
        for h in range(2):
            first_landed(h, 2)
            first_landed(h, 3)
            second_out(h, 4, 2)

    ring(1, 1)
    second_on(2)
    second_on(3)
    ring(2, 1)
    ring(0, 2)
    ring(1, 2)
    second_on(4)
    ring(2, 2)

    with scope("w_end"):
        for h in range(2):
            for place, j in offsets:
                second_landed(h, 2, place, j)
                second_landed(h, 3, place, j)
        landed(D1r.at[0 : N - 1], scr)
    for i in range(3):
        prepare(i)

    ring(0, 3)
    for i in range(3, L):
        prepare(i)
    ring(1, 3)
    ring(2, 3)

    with scope("p_on"):
        landed(PD.at[0 : N - 1], p2r)
        PE[slot] = PD[r]
        to_row(lambda p: rcopy(PD.at[p], PE.at[slot], pbs, pbr, row=p))

    ring(0, 4)
    ring(1, 4)
    ring_landed(0)
    dots_of(0)
    dots_of(1)
    ring(2, 4)
    ring_landed(1)
    dots_of(2)
    dots_of(3)
    ring_landed(2)
    dots_of(4)
    dots_of(5)

    with scope("d1send"):
        D1r[c] = DL[:, own]
        quick_col(lambda q: rcopy(DL.at[:, pl.ds(aligned(q, 128), 128)], D1r.at[c], d1s, d1r, col=q))
    for i in range(2):
        grads_of(i)

    with scope("u"):
        landed(PE.at[0 : N - 1], pbr)
        kind = lax.broadcasted_iota(jnp.int32, (256, 128), 0) % 16 // 2
        low = PE[...].reshape(N * 16, 256)
        inner_outer = jnp.zeros((256, 128), F32)
        for i in range(L):
            inner_outer = jnp.where(kind == i, nn(low, grads[i]), inner_outer)
        USb[:, 0:16, :] = inner_outer.astype(BF16).reshape(N, 16, 128)
        USr[slot] = USb[slot]
        to_row(lambda p: rcopy(USb.at[lax.rem(p, 2) * ZS + p // 2], USr.at[slot], uss, usr, row=p))

    for i in range(2, 4):
        grads_of(i)

    with scope("d1"):
        landed(D1r.at[0 : N - 1], d1r)
        sub = D1r[0]
        for p in range(1, N):
            sub = sub + D1r[p]
        landed(D1r.at[0 : N - 1], scs)
        SQ[...] = sub
        D2r[r] = sub
        quick_row(lambda p: rcopy(SQ, D2r.at[r], d2s, d2r, row=p))

    for i in range(4, L):
        grads_of(i)
    stores = [
        pltpu.make_async_copy(o_in, h_in, out_s.at[0]),
        pltpu.make_async_copy(o_mag, h_mag_grad, out_s.at[1]),
        pltpu.make_async_copy(o_ain, h_ain_grad, out_s.at[2]),
        pltpu.make_async_copy(o_aout, h_aout_grad, out_s.at[3]),
    ]
    stores[0].start()
    with scope("irsend"):
        IRr[c] = IPf[pl.ds(aligned(c, 16), 16), :]
        to_col(lambda q: rcopy(IPf.at[pl.ds(aligned(q, 16), 16), :], IRr.at[c], irs, irr, col=q))

    with scope("drain0"):
        for g in range(NG):
            landed(H.at[0 : N - 1, layers(g)], t1s.at[g])
            landed(H.at[0 : N - 1, layers(g)], t2s.at[g])
            for s in range(4):
                right(g, s).wait_send()
                left(g, s).wait_send()
            for n, i in enumerate(hops):
                over(g, n, i).wait_send()
        for h in range(2):
            for n, j in enumerate((0, 0, -1, 1)):
                first(h, n, j).wait_send()
            for place, j in offsets:
                for n, jb in enumerate((0, 0, -1, 1)):
                    second(h, n, place, j, jb).wait_send()
        landed(PPr.at[0 : ZS - 1], p1s)
        landed(PD.at[0 : N - 1], p2s)
        landed(PD.at[0 : N - 1], pbs)

    with scope("us"):
        landed(USr.at[0 : N - 1], usr)
        both = USr[0].astype(F32)
        for p in range(1, N):
            both = both + USr[p].astype(F32)

    with scope("d2"):
        landed(D2r.at[0 : N - 1], d2r)
        dots8 = D2r[0]
        for p in range(1, N):
            dots8 = dots8 + D2r[p]
        dots = dots8[0:L]
        o_mag[...] = dots / norms
        stores[1].start()
        correct = minus * dots
        for i in range(L):
            CR[i : i + 1, own] = correct[i : i + 1]
        landed(D1r.at[0 : N - 1], d1s)
        landed(D2r.at[0 : N - 1], d2s)
        SQ[0:L] = correct
        quick_col(lambda q: rcopy(SQ, CR.at[:, own], d3s, d3r, col=q))
        out = jnp.zeros((16, 128), F32)
        kind16 = lax.broadcasted_iota(jnp.int32, (16, 128), 0) // 2
        for i in range(L):
            out = jnp.where(kind16 == i, both[0:16] * scales[i : i + 1] + both[16:32] * correct[i : i + 1], out)
        OGr[pl.ds(aligned(slot, 16), 16), :] = out
        ranks_out = OGr.at[pl.ds(aligned(slot, 16), 16), :]
        to_row(lambda p: rcopy(ranks_out, ranks_out, ogs, ogr, row=p))

    with scope("ir"):
        landed(IRr.at[0 : N - 1], irr)
        in_sum = IRr[0]
        for p in range(1, N):
            in_sum = in_sum + IRr[p]
        IAr[pl.ds(aligned(c, 16), 16), :] = in_sum
        block = IAr.at[pl.ds(aligned(c, 16), 16), :]
        to_col(lambda q: rcopy(block, block, ias, iar, col=q))

    with scope("d3"):
        landed(D1r.at[0 : N - 1], d3r)
    with scope("term2"):
        for i in range(L):
            second_term = jnp.zeros((128, 32), F32)
            for n in range(NCH):
                cols = pl.ds(n * CH, CH)
                scaled_out = (WA[i, 128:160, cols].astype(F32) * CR[i : i + 1, cols]).astype(BF16)
                second_term += nt(WM[i, 0:128, cols], scaled_out)
            o_ain[i] = jnp.transpose(second_term)

    with scope("og"):
        landed(OGr.at[0 : 240, :], ogr)
        for i in range(L):
            for q in range(2):
                o_aout[i, pl.ds(q, N, stride=2), :] = OGr[pl.ds(2 * i + q, N, stride=16), :]
        stores[3].start()

    with scope("ia"):
        landed(IAr.at[0 : 240, :], iar)
        for i in range(L):
            for q in range(2):
                o_ain[i, pl.ds(q, N, stride=2), :] += IAr[pl.ds(2 * i + q, N, stride=16), :]
        stores[2].start()

    with scope("drain"):
        landed(USr.at[0 : N - 1], uss)
        landed(D1r.at[0 : N - 1], d3s)
        landed(OGr.at[0 : 240, :], ogs)
        landed(IRr.at[0 : N - 1], irs)
        landed(IAr.at[0 : 240, :], ias)
        for store in stores:
            store.wait()


def results(a, b, d, e, oa, ob, od, oe, va, vb, vd, ve, sems):
    into = []
    away = []
    for n, (have, held, out) in enumerate(((a, va, oa), (b, vb, ob), (d, vd, od), (e, ve, oe))):
        into.append(pltpu.make_async_copy(have, held, sems.at[n]))
        away.append(pltpu.make_async_copy(held, out, sems.at[4 + n]))
    for copy in into:
        copy.start()
    for n in range(4):
        into[n].wait()
        away[n].start()
    for copy in away:
        copy.wait()


def body(attn_out, out_cotangent, frozen, adapt_in, adapt_out, magnitude):
    dma = pltpu.SemaphoreType.DMA
    hbm = pl.BlockSpec(memory_space=pltpu.HBM)
    V = pltpu.VMEM
    scratch = [
        V((L, 256, 128), BF16),
        V((L, 256, 128), BF16),
        V((L, 32, 128), BF16),
        V((L, 128), F32),
        V((L, 256, 128), BF16),
        V((L, 32, 128), F32),
        V((L, 32, 128), F32),
        V((L, 128), F32),
        V((N, L, 16, 128), BF16),
        V((L, 256, 2048), BF16),
        V((L, 160, 2048), BF16),
        V((L, 128, 2048), F32),
        V((L, 128, 2048), BF16),
        V((8, 128), F32),
        V((8, 128), F32),
        V((ZS, 8, 128), F32),
        V((8, 2048), F32),
        V((8, 2048), F32),
        V((N, 16, 256), F32),
        V((ZS, 16, 256), F32),
        V((ZS, 16, 256), BF16),
        V((ZS, 16, 256), BF16),
        V((16, 256), BF16),
        V((N, 16, 256), BF16),
        V((N, 16, 256), BF16),
        V((N, 32, 128), BF16),
        V((N, 32, 128), BF16),
        V((8, 2048), F32),
        V((N, 8, 128), F32),
        V((N, 8, 128), F32),
        V((N * 16, 128), F32),
        V((N * 16, 128), F32),
        V((N, 16, 128), F32),
        V((N * 16, 128), F32),
        V((32, 128), F32),
        dma((6,)), dma((4,)),
        dma((NG,)), dma((NG,)), dma((NG,)), dma((NG,)),
        dma((NG, 4)), dma((NG, 4)), dma((NG, 4)), dma((NG, 4)),
        dma((NG, 8)), dma((NG, 8)),
        dma((2, 5, 4)), dma((2, 5, 4)),
        dma, dma((2,)), dma, dma, dma, dma((2,)), dma, dma,
        dma, dma, dma, dma,
        dma, dma, dma, dma, dma, dma, dma, dma, dma, dma, dma, dma,
    ]
    shapes = (
        jax.ShapeDtypeStruct((L, 256, 128), BF16),
        jax.ShapeDtypeStruct((L, 32, 128), F32),
        jax.ShapeDtypeStruct((L, 32, 128), F32),
        jax.ShapeDtypeStruct((L, 128), F32),
    )
    found = pl.pallas_call(
        kernel,
        out_shape=shapes,
        in_specs=[hbm] * 6,
        out_specs=(hbm,) * 4,
        scratch_shapes=scratch,
        compiler_params=pltpu.CompilerParams(
            collective_id=0, has_side_effects=True, vmem_limit_bytes=67043328
        ),
        name="dora",
    )(attn_out, out_cotangent, adapt_in, magnitude, frozen, adapt_out)
    return pl.pallas_call(
        results,
        out_shape=shapes,
        in_specs=[hbm] * 4,
        out_specs=(hbm,) * 4,
        scratch_shapes=[V(shape.shape, shape.dtype) for shape in shapes] + [dma((8,))],
        compiler_params=pltpu.CompilerParams(vmem_limit_bytes=67043328),
        name="results",
    )(*found)

def solution(mesh):
    return jax.shard_map(
        body,
        mesh=mesh,
        in_specs=(
            P(None, "col", "row"),
            P(None, "row", "col"),
            P(None, "row", "col"),
            P(None, None, "row"),
            P(None, None, "col"),
            P(None, "col"),
        ),
        out_specs=(
            P(None, "col", "row"),
            P(None, None, "row"),
            P(None, None, "col"),
            P(None, "col"),
        ),
        check_vma=False,
    )
```

```python
import functools

import jax
import jax.numpy as jnp
from jax import lax
from jax.experimental import pallas as pl
from jax.experimental.pallas import tpu as pltpu
from jax.sharding import PartitionSpec as P

F32 = jnp.float32
BF16 = jnp.bfloat16
N = 16
ZS = 8
L = 6
NG = 3
GL = L // NG
CH = 512
NCH = 2048 // CH


def nn(a, b):
    return lax.dot_general(a, b, (((1,), (0,)), ((), ())), preferred_element_type=F32)


def nt(a, b):
    return lax.dot_general(a, b, (((1,), (1,)), ((), ())), preferred_element_type=F32)


def tn(a, b):
    return lax.dot_general(a, b, (((0,), (0,)), ((), ())), preferred_element_type=F32)


def aligned(i, n):
    return pl.multiple_of(i * n, n)


def kernel(
    h_acts, h_grads, h_ain, h_mag, h_frozen, h_aout,
    h_in, h_ain_grad, h_aout_grad, h_mag_grad,
    acts, grads, ain, mag, o_in, o_ain, o_aout, o_mag,
    H, G, WA, MF, WM, SQ, SQx, SQr, SC, CR, PPf, PPx, PPb, PPr, PSb, PD, PE, USb, USr, DL, D1r, D2r, OGr, IPf, IRr, IAr, TMP,
    in_s, out_s, t1s, t1r, t2s, t2r, rs, rr, ls, lr, ds, dr, ws, wr,
    sqs, sqr, scs, scr, p1s, p1r, p2s, p2r, pbs, pbr, uss, usr,
    d1s, d1r, d2s, d2r, d3s, d3r, ogs, ogr, irs, irr, ias, iar,
):
    r = lax.axis_index("row")
    c = lax.axis_index("col")
    z, k = r // 2, r % 2
    slot = k * ZS + z
    partner = z * 2 + 1 - k
    x, y = c // 4, c % 4
    scope = jax.named_scope

    def rcopy(src, dst, ss, rsem, **ids):
        return pltpu.make_async_remote_copy(
            src_ref=src, dst_ref=dst, send_sem=ss, recv_sem=rsem,
            device_id=ids, device_id_type=pl.DeviceIdType.MESH,
        )

    def landed(ref, sem):
        pltpu.make_async_copy(ref, ref, sem).wait()

    def to_row(make):
        def step(i, _):
            make(lax.rem(r + i, N)).start()
            return 0
        lax.fori_loop(1, N, step, 0)

    def to_col(make):
        def step(i, _):
            make(lax.rem(c + i, N)).start()
            return 0
        lax.fori_loop(1, N, step, 0)

    def quick_row(make):
        for i in (8, 7, 9, 6, 10, 5, 11, 4, 12, 3, 13, 2, 14, 1, 15):
            make(lax.rem(r + i, N)).start()

    def quick_col(make):
        for i in (10, 9, 11, 6, 14, 8, 2, 5, 7, 13, 15, 4, 12, 1, 3):
            make(lax.rem(x + i // 4, 4) * 4 + lax.rem(y + i % 4, 4)).start()

    own = pl.ds(aligned(c, 128), 128)
    mine = pl.ds(aligned(r, 16), 16)

    def layers(g):
        return pl.ds(GL * g, GL)

    loads = [
        pltpu.make_async_copy(h_grads, grads, in_s.at[0]),
        pltpu.make_async_copy(h_frozen, WA.at[:, 0:128, own], in_s.at[1]),
        pltpu.make_async_copy(h_aout, WA.at[:, 128:160, own], in_s.at[2]),
        pltpu.make_async_copy(h_ain, ain, in_s.at[3]),
        pltpu.make_async_copy(h_acts, acts, in_s.at[4]),
        pltpu.make_async_copy(h_mag, mag, in_s.at[5]),
    ]
    with scope("s00_barrier"):
        barrier = pltpu.get_barrier_semaphore()

        def greet(i, _):
            pl.semaphore_signal(barrier, inc=1, device_id={"row": lax.rem(r + i, N)}, device_id_type=pl.DeviceIdType.MESH)
            pl.semaphore_signal(barrier, inc=1, device_id={"col": lax.rem(c + i, N)}, device_id_type=pl.DeviceIdType.MESH)
            return 0

        lax.fori_loop(1, N, greet, 0)
        for load in loads:
            load.start()
        loads[0].wait()
        pl.semaphore_wait(barrier, 2 * (N - 1))

    with scope("s01_t1send"):
        for g in range(NG):
            to_row(lambda p, g=g: rcopy(
                grads.at[layers(g), pl.ds(aligned(p, 16), 16), :], H.at[r, layers(g)],
                t1s.at[g], t1r.at[g], row=p))

    for load in loads[1:]:
        load.wait()
    H[r] = grads[:, mine, :]

    def place_of(h, a, b):
        return 4 * b + a if h == 0 else 4 * a + b

    pos = ((y, x), (x, y))
    cuts = ((0, 160), (0, 160), (0, 80), (80, 160))

    def wblock(h, a, b, lo=0, hi=160):
        return WA.at[pl.ds(3 * h, 3), lo:hi, pl.ds(aligned(place_of(h, a, b), 128), 128)]

    def mod4(i):
        return lax.rem(i + 4, 4)

    def w_copy(h, kind, slot, a, b, target):
        ref = wblock(h, a, b, *cuts[kind])
        return rcopy(ref, ref, ws.at[h, slot, kind], wr.at[h, slot, kind], col=target)

    def first(h, kind, j):
        a, b = pos[h]
        step = 1 if kind in (0, 2) else -1
        return w_copy(h, kind, 0, mod4(a + j), b, place_of(h, mod4(a + step), b))

    def second(h, kind, slot, j, jb):
        a, b = pos[h]
        step = 1 if kind in (0, 2) else -1
        return w_copy(h, kind, slot, mod4(a + j), mod4(b + jb), place_of(h, a, mod4(b + step)))

    def first_landed(h, kind):
        a, b = pos[h]
        landed(wblock(h, mod4(a + (-1, 1, 2, 2)[kind]), b, *cuts[kind]), wr.at[h, 0, kind])

    def second_landed(h, kind, slot, j):
        a, b = pos[h]
        landed(wblock(h, mod4(a + j), mod4(b + (-1, 1, 2, 2)[kind]), *cuts[kind]), wr.at[h, slot, kind])

    offsets = ((1, 0), (2, -1), (3, 1), (4, 2))

    def second_out(h, slot, j):
        second(h, 0, slot, j, 0).start()
        second(h, 1, slot, j, 0).start()

    def second_on(slot):
        with scope(f"w_on{slot}"):
            j = dict(offsets)[slot]
            for h in range(2):
                second_landed(h, 0, slot, j)
                second(h, 2, slot, j, -1).start()
                second_landed(h, 1, slot, j)
                second(h, 3, slot, j, 1).start()

    for h in range(2):
        first(h, 0, 0).start()
        first(h, 1, 0).start()
    for h in range(2):
        second_out(h, 1, 0)

    rows = lax.broadcasted_iota(jnp.int32, (256, 32), 0)
    ranks = lax.broadcasted_iota(jnp.int32, (256, 32), 1)

    def spread(i):
        off = rows % 16 - 2 * i
        return jnp.where((off >= 0) & (off < 2) & (ranks == rows // 16 * 2 + off), 1.0, 0.0).astype(F32)

    with scope("s02_local"):
        SQ[...] = jnp.zeros((8, 128), F32)
        part = jnp.zeros((256, 256), F32)
        inner = jnp.zeros((256, 128), F32)
        for i in range(L):
            block = WA[i, 0:128, own].astype(F32) + tn(ain[i], WA[i, 128:160, own])
            SQ[i : i + 1] = jnp.sum(block * block, axis=0, keepdims=True)
            wide = nn(spread(i).astype(BF16), ain[i]).astype(BF16)
            part += nt(wide, acts[i])
            high = block.astype(BF16)
            inner += nn(wide, high) + nn(wide, (block - high.astype(F32)).astype(BF16))
        PPf[...] = part.reshape(N, 16, 256)
        USb[:, 16:32, :] = inner.astype(BF16).reshape(N, 16, 128)
        theirs = pl.ds(aligned(1 - k, ZS), ZS)
        to_partner = [
            rcopy(SQ, SQx, sqs, sqr.at[0], row=partner),
            rcopy(PPf.at[theirs], PPx, p1s, p1r.at[0], row=partner),
        ]
        for copy in to_partner:
            copy.start()

    def to_column(make):
        def step(i, _):
            make(lax.rem(z + i, ZS)).start()
            return 0
        lax.fori_loop(1, ZS, step, 0)

    with scope("pairs"):
        for copy in to_partner:
            copy.wait()
        SQ[...] = SQ[...] + SQx[...]
        SQr[z] = SQ[...]
        to_column(lambda q: rcopy(SQ, SQr.at[z], sqs, sqr.at[1], row=q * 2 + k))
        PPb[...] = (PPf[pl.ds(aligned(k, ZS), ZS)] + PPx[...]).astype(BF16)
        PPr[z] = PPb[z]
        to_column(lambda q: rcopy(PPb.at[q], PPr.at[z], p1s, p1r.at[1], row=q * 2 + k))

    def exchange(g):
        with scope(f"t2_{g}"):
            landed(H.at[0 : N - 1, layers(g)], t1r.at[g])
            to_col(lambda q: rcopy(
                H.at[q, layers(g)], G.at[layers(g), mine, own], t2s.at[g], t2r.at[g], col=q))
            G[GL * g : GL * g + GL, mine, own] = H[c, GL * g : GL * g + GL]

    def chunk(g, q, count=GL, at=0):
        return G.at[pl.ds(GL * g + at, count), pl.ds(aligned(q, 16), 16), :]

    def across(i):
        return lax.rem(z + i + ZS, ZS) * 2 + k

    def right(g, s):
        ref = chunk(g, across(-s)) if s < 3 else chunk(g, across(-s), 1, 0)
        return rcopy(ref, ref, rs.at[g, s], rr.at[g, s], row=across(1))

    def left(g, s):
        ref = chunk(g, across(s)) if s < 3 else chunk(g, across(s), 1, 1)
        return rcopy(ref, ref, ls.at[g, s], lr.at[g, s], row=across(-1))

    def over(g, n, i):
        ref = chunk(g, across(i), *parts[n])
        return rcopy(ref, ref, ds.at[g, n], dr.at[g, n], row=partner)

    hops = (0, -1, -2, -3, 1, 2, 3, 4, 4)
    parts = ((GL, 0),) * 7 + ((1, 0), (1, 1))

    def ring(g, s):
        with scope(f"r{g}{s}"):
            if s == 0:
                landed(G.at[layers(g), mine, 0 : 128 * (N - 1)], t2r.at[g])
                right(g, 0).start()
                left(g, 0).start()
                over(g, 0, 0).start()
            elif s < 4:
                landed(chunk(g, across(-s)), rr.at[g, s - 1])
                right(g, s).start()
                landed(chunk(g, across(s)), lr.at[g, s - 1])
                left(g, s).start()
                over(g, s, -s).start()
                over(g, 3 + s, s).start()
            else:
                landed(chunk(g, across(4), 1, 0), rr.at[g, 3])
                over(g, 7, 4).start()
                landed(chunk(g, across(4), 1, 1), lr.at[g, 3])
                over(g, 8, 4).start()

    def ring_landed(g):
        with scope(f"r{g}_landed"):
            for n, i in enumerate(hops):
                landed(chunk(g, lax.rem(z + i + ZS, ZS) * 2 + 1 - k, *parts[n]), dr.at[g, n])

    def prepare(i):
        with scope(f"prep{i}"):
            for n in range(NCH):
                cols = pl.ds(n * CH, CH)
                merged = WA[i, 0:128, cols].astype(F32) + tn(ain[i], WA[i, 128:160, cols])
                MF[i, :, cols] = merged
                WM[i, :, cols] = merged.astype(BF16)

    def dots_of(i):
        with scope(f"dots{i}"):
            for n in range(NCH):
                cols = pl.ds(n * CH, CH)
                outer = tn(acts[i], G[i, :, cols])
                DL[i : i + 1, cols] = jnp.sum(MF[i, :, cols] * outer, axis=0, keepdims=True)

    def grads_of(i):
        with scope(f"grads{i}"):
            got = jnp.zeros((256, 128), F32)
            low_t = jnp.zeros((32, 256), F32)
            for n in range(NCH):
                cols = pl.ds(n * CH, CH)
                scaled = (G[i, :, cols].astype(F32) * SC[i : i + 1, cols]).astype(BF16)
                got += nt(scaled, WM[i, :, cols])
                low_t += nt(WA[i, 128:160, cols], scaled)
            o_in[i] = got.astype(BF16)
            high = low_t.astype(BF16)
            rest = (low_t - high.astype(F32)).astype(BF16)
            TMP[...] = nn(high, acts[i]) + nn(rest, acts[i])
            for q in range(2):
                IPf[pl.ds(2 * i + q, N, stride=16), :] = TMP[pl.ds(q, N, stride=2), :]

    DL[...] = jnp.zeros((8, 2048), F32)
    IPf[...] = jnp.zeros((N * 16, 128), F32)

    exchange(0)
    exchange(1)

    with scope("w_first"):
        for h in range(2):
            first_landed(h, 0)
            first(h, 2, -1).start()
            first_landed(h, 1)
            first(h, 3, 1).start()

    ring(0, 0)
    exchange(2)
    for h in range(2):
        second_out(h, 2, -1)
        second_out(h, 3, 1)
    second_on(1)
    ring(1, 0)

    with scope("norms"):
        landed(SQr.at[0 : ZS - 1], sqr.at[1])
        squares = SQr[0]
        for p in range(1, ZS):
            squares = squares + SQr[p]
        norms = jnp.sqrt(squares[0:L] + 0.25)
        scales = mag[...] / norms
        minus = -mag[...] / (norms * norms * norms)
        for i in range(L):
            SC[i : i + 1, own] = scales[i : i + 1]
        landed(SQr.at[0 : ZS - 1], sqs)
        SQ[0:L] = scales
        to_col(lambda q: rcopy(SQ, SC.at[:, own], scs, scr, col=q))

    ring(0, 1)

    with scope("psum"):
        landed(PPr.at[0 : ZS - 1], p1r.at[1])
        total = PPr[0].astype(F32)
        for p in range(1, ZS):
            total = total + PPr[p].astype(F32)
        PSb[...] = total.astype(BF16)
        PD[c] = PSb[...]
        to_col(lambda q: rcopy(PSb, PD.at[c], p2s, p2r, col=q))

    ring(2, 0)

    with scope("w_first2"):
        for h in range(2):
            first_landed(h, 2)
            first_landed(h, 3)
            second_out(h, 4, 2)

    ring(1, 1)
    second_on(2)
    second_on(3)
    ring(2, 1)
    ring(0, 2)
    ring(1, 2)
    second_on(4)
    ring(2, 2)

    with scope("w_end"):
        for h in range(2):
            for place, j in offsets:
                second_landed(h, 2, place, j)
                second_landed(h, 3, place, j)
        landed(D1r.at[0 : N - 1], scr)
    for i in range(3):
        prepare(i)

    ring(0, 3)
    for i in range(3, L):
        prepare(i)
    ring(1, 3)
    ring(2, 3)

    with scope("p_on"):
        landed(PD.at[0 : N - 1], p2r)
        PE[slot] = PD[r]
        to_row(lambda p: rcopy(PD.at[p], PE.at[slot], pbs, pbr, row=p))

    ring(0, 4)
    ring(1, 4)
    ring_landed(0)
    dots_of(0)
    dots_of(1)
    ring(2, 4)
    ring_landed(1)
    dots_of(2)
    dots_of(3)
    ring_landed(2)
    dots_of(4)
    dots_of(5)

    with scope("d1send"):
        D1r[c] = DL[:, own]
        quick_col(lambda q: rcopy(DL.at[:, pl.ds(aligned(q, 128), 128)], D1r.at[c], d1s, d1r, col=q))
    for i in range(2):
        grads_of(i)

    with scope("u"):
        landed(PE.at[0 : N - 1], pbr)
        kind = lax.broadcasted_iota(jnp.int32, (256, 128), 0) % 16 // 2
        low = PE[...].reshape(N * 16, 256)
        inner_outer = jnp.zeros((256, 128), F32)
        for i in range(L):
            inner_outer = jnp.where(kind == i, nn(low, grads[i]), inner_outer)
        USb[:, 0:16, :] = inner_outer.astype(BF16).reshape(N, 16, 128)
        USr[slot] = USb[slot]
        to_row(lambda p: rcopy(USb.at[lax.rem(p, 2) * ZS + p // 2], USr.at[slot], uss, usr, row=p))

    for i in range(2, 4):
        grads_of(i)

    with scope("d1"):
        landed(D1r.at[0 : N - 1], d1r)
        sub = D1r[0]
        for p in range(1, N):
            sub = sub + D1r[p]
        landed(D1r.at[0 : N - 1], scs)
        SQ[...] = sub
        D2r[r] = sub
        quick_row(lambda p: rcopy(SQ, D2r.at[r], d2s, d2r, row=p))

    for i in range(4, L):
        grads_of(i)
    stores = [
        pltpu.make_async_copy(o_in, h_in, out_s.at[0]),
        pltpu.make_async_copy(o_mag, h_mag_grad, out_s.at[1]),
        pltpu.make_async_copy(o_ain, h_ain_grad, out_s.at[2]),
        pltpu.make_async_copy(o_aout, h_aout_grad, out_s.at[3]),
    ]
    stores[0].start()
    with scope("irsend"):
        IRr[c] = IPf[pl.ds(aligned(c, 16), 16), :]
        quick_col(lambda q: rcopy(IPf.at[pl.ds(aligned(q, 16), 16), :], IRr.at[c], irs, irr, col=q))

    with scope("drain0"):
        for g in range(NG):
            landed(H.at[0 : N - 1, layers(g)], t1s.at[g])
            landed(H.at[0 : N - 1, layers(g)], t2s.at[g])
            for s in range(4):
                right(g, s).wait_send()
                left(g, s).wait_send()
            for n, i in enumerate(hops):
                over(g, n, i).wait_send()
        for h in range(2):
            for n, j in enumerate((0, 0, -1, 1)):
                first(h, n, j).wait_send()
            for place, j in offsets:
                for n, jb in enumerate((0, 0, -1, 1)):
                    second(h, n, place, j, jb).wait_send()
        landed(PPr.at[0 : ZS - 1], p1s)
        landed(PD.at[0 : N - 1], p2s)
        landed(PD.at[0 : N - 1], pbs)

    with scope("us"):
        landed(USr.at[0 : N - 1], usr)
        both = USr[0].astype(F32)
        for p in range(1, N):
            both = both + USr[p].astype(F32)

    with scope("d2"):
        landed(D2r.at[0 : N - 1], d2r)
        dots8 = D2r[0]
        for p in range(1, N):
            dots8 = dots8 + D2r[p]
        dots = dots8[0:L]
        o_mag[...] = dots / norms
        stores[1].start()
        correct = minus * dots
        for i in range(L):
            CR[i : i + 1, own] = correct[i : i + 1]
        landed(D1r.at[0 : N - 1], d1s)
        landed(D2r.at[0 : N - 1], d2s)
        SQ[0:L] = correct
        quick_col(lambda q: rcopy(SQ, CR.at[:, own], d3s, d3r, col=q))
        out = jnp.zeros((16, 128), F32)
        kind16 = lax.broadcasted_iota(jnp.int32, (16, 128), 0) // 2
        for i in range(L):
            out = jnp.where(kind16 == i, both[0:16] * scales[i : i + 1] + both[16:32] * correct[i : i + 1], out)
        OGr[pl.ds(aligned(slot, 16), 16), :] = out
        ranks_out = OGr.at[pl.ds(aligned(slot, 16), 16), :]
        quick_row(lambda p: rcopy(ranks_out, ranks_out, ogs, ogr, row=p))

    with scope("ir"):
        landed(IRr.at[0 : N - 1], irr)
        in_sum = IRr[0]
        for p in range(1, N):
            in_sum = in_sum + IRr[p]
        IAr[pl.ds(aligned(c, 16), 16), :] = in_sum
        block = IAr.at[pl.ds(aligned(c, 16), 16), :]
        quick_col(lambda q: rcopy(block, block, ias, iar, col=q))

    with scope("d3"):
        landed(D1r.at[0 : N - 1], d3r)
    with scope("term2"):
        for i in range(L):
            second_term = jnp.zeros((128, 32), F32)
            for n in range(NCH):
                cols = pl.ds(n * CH, CH)
                scaled_out = (WA[i, 128:160, cols].astype(F32) * CR[i : i + 1, cols]).astype(BF16)
                second_term += nt(WM[i, 0:128, cols], scaled_out)
            o_ain[i] = jnp.transpose(second_term)

    with scope("og"):
        landed(OGr.at[0 : 240, :], ogr)
        for i in range(L):
            for q in range(2):
                o_aout[i, pl.ds(q, N, stride=2), :] = OGr[pl.ds(2 * i + q, N, stride=16), :]
        stores[3].start()

    with scope("ia"):
        landed(IAr.at[0 : 240, :], iar)
        for i in range(L):
            for q in range(2):
                o_ain[i, pl.ds(q, N, stride=2), :] += IAr[pl.ds(2 * i + q, N, stride=16), :]
        stores[2].start()

    with scope("drain"):
        landed(USr.at[0 : N - 1], uss)
        landed(D1r.at[0 : N - 1], d3s)
        landed(OGr.at[0 : 240, :], ogs)
        landed(IRr.at[0 : N - 1], irs)
        landed(IAr.at[0 : 240, :], ias)
        for store in stores:
            store.wait()


def results(a, b, d, e, oa, ob, od, oe, va, vb, vd, ve, sems):
    into = []
    away = []
    for n, (have, held, out) in enumerate(((a, va, oa), (b, vb, ob), (d, vd, od), (e, ve, oe))):
        into.append(pltpu.make_async_copy(have, held, sems.at[n]))
        away.append(pltpu.make_async_copy(held, out, sems.at[4 + n]))
    for copy in into:
        copy.start()
    for n in range(4):
        into[n].wait()
        away[n].start()
    for copy in away:
        copy.wait()


def body(attn_out, out_cotangent, frozen, adapt_in, adapt_out, magnitude):
    dma = pltpu.SemaphoreType.DMA
    hbm = pl.BlockSpec(memory_space=pltpu.HBM)
    V = pltpu.VMEM
    scratch = [
        V((L, 256, 128), BF16),
        V((L, 256, 128), BF16),
        V((L, 32, 128), BF16),
        V((L, 128), F32),
        V((L, 256, 128), BF16),
        V((L, 32, 128), F32),
        V((L, 32, 128), F32),
        V((L, 128), F32),
        V((N, L, 16, 128), BF16),
        V((L, 256, 2048), BF16),
        V((L, 160, 2048), BF16),
        V((L, 128, 2048), F32),
        V((L, 128, 2048), BF16),
        V((8, 128), F32),
        V((8, 128), F32),
        V((ZS, 8, 128), F32),
        V((8, 2048), F32),
        V((8, 2048), F32),
        V((N, 16, 256), F32),
        V((ZS, 16, 256), F32),
        V((ZS, 16, 256), BF16),
        V((ZS, 16, 256), BF16),
        V((16, 256), BF16),
        V((N, 16, 256), BF16),
        V((N, 16, 256), BF16),
        V((N, 32, 128), BF16),
        V((N, 32, 128), BF16),
        V((8, 2048), F32),
        V((N, 8, 128), F32),
        V((N, 8, 128), F32),
        V((N * 16, 128), F32),
        V((N * 16, 128), F32),
        V((N, 16, 128), F32),
        V((N * 16, 128), F32),
        V((32, 128), F32),
        dma((6,)), dma((4,)),
        dma((NG,)), dma((NG,)), dma((NG,)), dma((NG,)),
        dma((NG, 4)), dma((NG, 4)), dma((NG, 4)), dma((NG, 4)),
        dma((NG, 9)), dma((NG, 9)),
        dma((2, 5, 4)), dma((2, 5, 4)),
        dma, dma((2,)), dma, dma, dma, dma((2,)), dma, dma,
        dma, dma, dma, dma,
        dma, dma, dma, dma, dma, dma, dma, dma, dma, dma, dma, dma,
    ]
    shapes = (
        jax.ShapeDtypeStruct((L, 256, 128), BF16),
        jax.ShapeDtypeStruct((L, 32, 128), F32),
        jax.ShapeDtypeStruct((L, 32, 128), F32),
        jax.ShapeDtypeStruct((L, 128), F32),
    )
    found = pl.pallas_call(
        kernel,
        out_shape=shapes,
        in_specs=[hbm] * 6,
        out_specs=(hbm,) * 4,
        scratch_shapes=scratch,
        compiler_params=pltpu.CompilerParams(
            collective_id=0, has_side_effects=True, vmem_limit_bytes=67043328
        ),
        name="dora",
    )(attn_out, out_cotangent, adapt_in, magnitude, frozen, adapt_out)
    return pl.pallas_call(
        results,
        out_shape=shapes,
        in_specs=[hbm] * 4,
        out_specs=(hbm,) * 4,
        scratch_shapes=[V(shape.shape, shape.dtype) for shape in shapes] + [dma((8,))],
        compiler_params=pltpu.CompilerParams(vmem_limit_bytes=67043328),
        name="results",
    )(*found)

def solution(mesh):
    return jax.shard_map(
        body,
        mesh=mesh,
        in_specs=(
            P(None, "col", "row"),
            P(None, "row", "col"),
            P(None, "row", "col"),
            P(None, None, "row"),
            P(None, None, "col"),
            P(None, "col"),
        ),
        out_specs=(
            P(None, "col", "row"),
            P(None, None, "row"),
            P(None, None, "col"),
            P(None, "col"),
        ),
        check_vma=False,
    )
```
